128 devices in a mesh: dp: 64 (over z, y, x), tensor: 2 (over core).
Axes of the slice: x: 4, y: 4, z: 4, core: 2. Of those that a mesh axis runs over, the one named last changes fastest.
Arguments:
- current: float32 [128, 4096], P('dp'), may hold values from -6 to 6
- noise_draw: float32 [128, 4096], P('dp'), may hold values from -6 to 6
- labels: bfloat16 [128, 1152], P('dp'), may hold values from -6 to 6
- time_now: float32 [128], P('dp'), may hold values from 0.4 to 1
- step_size: float32 [128], P('dp'), may hold values from 0.005 to 0.02
- accept: int32 [128], P('dp'), may hold values 0 or 1
- patch_weight: bfloat16 [16, 1152], replicated, may hold values from -1.5 to 1.5
- time_in: bfloat16 [256, 1152], replicated, may hold values from -0.375 to 0.375
- time_out: bfloat16 [1152, 1152], replicated, may hold values from -0.1875 to 0.1875
- qkv_weight: bfloat16 [1, 1152, 3, 1152], P(None, None, None, 'tensor'), may hold values from -1 to 1
- out_weight: bfloat16 [1, 1152, 1152], P(None, None, 'tensor'), may hold values from -0.1875 to 0.1875
- ada_weight: bfloat16 [1, 1152, 3456], P(None, 'dp', 'tensor'), may hold values from -0.1875 to 0.1875
- final_ada: bfloat16 [1152, 2304], P('dp', 'tensor'), may hold values from -0.1875 to 0.1875
- final_proj: bfloat16 [1152, 16], replicated, may hold values from -0.1875 to 0.1875
Outputs:
- next_state: float32 [128, 4096], P('dp')
- error_norm: float32 [128], P('dp')
The draws below stay inside these ranges and needn't reach their ends.
All inputs are finite; a program needn't handle non-finite values. No bound on the sum of `accept` on one device may be relied on, other than what follows from the above.
Results may differ from the reference program's by a relative error of at most 0.015.
Values may be sent and summed in bfloat16 or wider, within the bound.
A program may use at most 128 MiB of HBM per device.

```python
import math
import jax
import jax.numpy as jnp
from jax import lax

D = 1152
HEADS = 16
TOK = 256
FREQ = 256
PATCH_VALS = 16
LAYERS = 1
HEAD_DIM = 72
LATENT = 4096
BATCH = 128
N_TENSOR = 2


def draw_qkv_weight(key, part):
    key_one = jax.random.fold_in(jax.random.fold_in(key, 17), 0)
    spread = D ** (-0.5)
    whole = jax.random.normal(key_one, (LAYERS, D, 3, D), jnp.float32) * spread
    return jnp.clip(whole, -1.0, 1.0).astype(jnp.bfloat16)


def plant(result, rng, low, top_value):
    longest = result.shape.index(max(result.shape))
    spots = []
    for shift in (0, 1):
        where = [jax.random.randint(jax.random.fold_in(rng, axis), (), 0, length) for axis, length in enumerate(result.shape)]
        where[longest] = (where[longest] + shift) % result.shape[longest]
        spots.append(tuple(where))
    return result.at[spots[0]].set(low).at[spots[1]].set(top_value)


def block_levels(stream_key, dims, pieces, low, top_value):
    factor_of, own = 1.0, jax.random.fold_in(stream_key, 6)
    for axis_at, blocks in pieces:
        heights = jnp.exp(jax.random.uniform(jax.random.fold_in(own, axis_at), (blocks,), jnp.float32, low / len(pieces), top_value / len(pieces)))
        factor_of = factor_of * jnp.repeat(heights, dims[axis_at] // blocks).reshape([-1 if axis == axis_at else 1 for axis in range(len(dims))])
    return factor_of


def scatter_about(own_key, extent, scale, bound, shards=(), kind=jnp.bfloat16):
    level = block_levels(own_key, extent, shards, -0.22, 0.18) if shards else 1.0
    result = jax.random.normal(own_key, extent, jnp.float32) * scale * level
    return jnp.minimum(jnp.maximum(result, -bound), bound).astype(kind)


def setup_inputs(seed: int = 0) -> dict:
    seeds = jax.random.split(jax.random.key(seed), 15)
    return {
        "current": scatter_about(seeds[0], (BATCH, LATENT), 1.0, 6.0, ((0, 64),), jnp.float32),
        "noise_draw": scatter_about(seeds[1], (BATCH, LATENT), 1.0, 6.0, ((0, 64),), jnp.float32),
        "labels": scatter_about(seeds[2], (BATCH, D), 1.0, 6.0, ((0, 64),)),
        "time_now": jnp.clip(0.4 + 0.6 * jax.random.uniform(seeds[3], (BATCH,), jnp.float32) ** block_levels(seeds[3], (BATCH,), ((0, 64),), -0.2, 0.2), 0.4, 1.0),
        "step_size": jnp.clip(0.005 + 0.015 * jax.random.uniform(seeds[4], (BATCH,), jnp.float32) ** block_levels(seeds[4], (BATCH,), ((0, 64),), -0.2, 0.2), 0.005, 0.02),
        "accept": plant((jax.random.randint(seeds[5], (BATCH,), 0, 4) < 3).astype(jnp.int32), jax.random.fold_in(seeds[5], 1), 0, 1),
        "patch_weight": scatter_about(seeds[6], (PATCH_VALS, D), PATCH_VALS ** -0.5, 1.5),
        "time_in": scatter_about(seeds[7], (FREQ, D), FREQ ** -0.5, 0.375),
        "time_out": scatter_about(seeds[8], (D, D), D ** -0.5, 0.1875),
        "qkv_weight": draw_qkv_weight(jax.random.fold_in(seeds[14], 71), 0),
        "out_weight": scatter_about(seeds[10], (LAYERS, D, D), D ** -0.5, 0.1875, ((2, 2),)),
        "ada_weight": scatter_about(seeds[11], (LAYERS, D, 3 * D), D ** -0.5, 0.1875, ((1, 64), (2, 2))),
        "final_ada": scatter_about(seeds[12], (D, 2 * D), D ** -0.5, 0.1875, ((0, 64), (1, 2))),
        "final_proj": scatter_about(seeds[13], (D, PATCH_VALS), D ** -0.5, 0.1875),
    }


beta_low = 0.1
beta_high = 20.0
tol_abs = 0.0078
tol_rel = 0.05
norm_eps = 1e-06

def beta_at(moments):
    return beta_low + (beta_high - beta_low) * moments

def sigma_at(moments):
    integral = beta_low * moments + 0.5 * (beta_high - beta_low) * moments * moments
    return jnp.sqrt(1.0 - jnp.exp(-integral))

def time_features(moments, feature_count):
    half_count = feature_count // 2
    freq_index = jnp.arange(half_count, dtype=jnp.float32)
    freq_rates = jnp.exp(-math.log(10000.0) * freq_index / half_count)
    angles = 1000.0 * moments[:, None] * freq_rates[None, :]
    return jnp.concatenate([jnp.cos(angles), jnp.sin(angles)], axis=1)

def position_table(positions, feature_count):
    half_count = feature_count // 2
    freq_index = jnp.arange(half_count, dtype=jnp.float32)
    freq_rates = jnp.exp(-math.log(10000.0) * freq_index / half_count)
    angles = positions.astype(jnp.float32)[:, None] * freq_rates[None, :]
    return jnp.concatenate([jnp.sin(angles), jnp.cos(angles)], axis=1)

def condition(moments, labels, time_in, time_out):
    features = time_features(moments, time_in.shape[0]).astype(jnp.bfloat16)
    hidden = jax.nn.silu(jnp.dot(features, time_in, preferred_element_type=jnp.float32)).astype(jnp.bfloat16)
    joined = labels.astype(jnp.float32) + jnp.dot(hidden, time_out, preferred_element_type=jnp.float32)
    return jax.nn.silu(joined).astype(jnp.bfloat16)

def layer_norm(values):
    average = lax.optimization_barrier(jnp.mean(values, axis=-1, keepdims=True))
    centred = values - average
    spread_sq = lax.optimization_barrier(jnp.mean(centred * centred, axis=-1, keepdims=True))
    return centred * lax.rsqrt(spread_sq + norm_eps)

def modulate(values, shift_vec, scale_vec):
    return (layer_norm(values) * (1.0 + scale_vec) + shift_vec).astype(jnp.bfloat16)

def rounded(values):
    return lax.optimization_barrier(values.astype(jnp.bfloat16)).astype(jnp.float32)

def drift(values, moments, noise_guess):
    beta_rate = beta_at(moments)[:, None]
    return 0.5 * beta_rate * values - beta_rate * noise_guess / sigma_at(moments)[:, None]

def denoise(latents, moments, labels, patch_weight, time_in, time_out, qkv_weight, out_weight, ada_weight, final_ada, final_proj):
    cond_act = condition(moments, labels, time_in, time_out)
    layer_mods = jnp.stack([jnp.dot(cond_act, ada_weight[block_index], preferred_element_type=jnp.float32) for block_index in range(LAYERS)], axis=1)
    final_mods = jnp.dot(cond_act, final_ada, preferred_element_type=jnp.float32)
    positions = position_table(jnp.arange(TOK, dtype=jnp.int32), D)
    groups = N_TENSOR
    highest = lax.Precision.HIGHEST

    def one_latent(inputs):
        latent, mod_rows, final_rows = inputs
        tokens = latent.reshape(TOK, PATCH_VALS).astype(jnp.bfloat16)
        stream = jnp.dot(tokens, patch_weight, preferred_element_type=jnp.float32) + positions
        for block_index in range(LAYERS):
            shift_attn, scale_attn, gate_attn = jnp.split(mod_rows[block_index], 3)
            attn_in = modulate(stream, shift_attn, scale_attn)
            projected = jnp.dot(attn_in, qkv_weight[block_index].reshape(D, 3 * D), preferred_element_type=jnp.float32)
            projected = rounded(projected).reshape(TOK, 3, HEADS, HEAD_DIM)
            scores = jnp.einsum('qhe,khe->hqk', projected[:, 0], projected[:, 1], precision=highest) * HEAD_DIM ** (-0.5)
            attn_probs = rounded(jax.nn.softmax(scores, axis=-1))
            attended = rounded(jnp.einsum('hqk,khe->qhe', attn_probs, projected[:, 2], precision=highest))
            attended = attended.reshape(TOK, groups, D // groups)
            out_groups = out_weight[block_index].reshape(D, groups, D // groups).astype(jnp.float32)
            partial_value = rounded(jnp.einsum('qgk,dgk->gqd', attended, out_groups, precision=highest))
            stream = stream + gate_attn * lax.optimization_barrier(jnp.sum(partial_value, axis=0))
        shift_final, scale_final = jnp.split(final_rows, 2)
        final_in = modulate(stream, shift_final, scale_final)
        return jnp.dot(final_in, final_proj, preferred_element_type=jnp.float32).reshape(LATENT)
    return lax.map(one_latent, (latents, layer_mods, final_mods))

def reference(current, noise_draw, labels, time_now, step_size, accept, patch_weight, time_in, time_out, qkv_weight, out_weight, ada_weight, final_ada, final_proj):
    noise_now = denoise(current, time_now, labels, patch_weight, time_in, time_out, qkv_weight, out_weight, ada_weight, final_ada, final_proj)
    drift_now = drift(current, time_now, noise_now)
    spread = jnp.sqrt(step_size * beta_at(time_now))[:, None] * noise_draw
    euler_state = current + step_size[:, None] * drift_now + spread
    later_time = time_now - step_size
    noise_later = denoise(euler_state, later_time, labels, patch_weight, time_in, time_out, qkv_weight, out_weight, ada_weight, final_ada, final_proj)
    drift_later = drift(euler_state, later_time, noise_later)
    heun_state = current + 0.5 * step_size[:, None] * (drift_now + drift_later) + spread
    scale_ref = jnp.maximum(tol_abs, tol_rel * jnp.maximum(jnp.abs(heun_state), jnp.abs(current)))
    scaled_gap = (euler_state - heun_state) / scale_ref
    error_norm = jnp.sqrt(lax.optimization_barrier(jnp.sum(scaled_gap * scaled_gap, axis=1)) / LATENT)
    next_state = jnp.where(accept[:, None] == 1, heun_state, current)
    return (next_state, error_norm)
```

```python
import functools
import math

import jax
import jax.numpy as jnp
from jax import lax
from jax.experimental import pallas as pl
from jax.experimental.pallas import tpu as pltpu
from jax.sharding import PartitionSpec as P

MESH = pl.DeviceIdType.MESH
F32 = jnp.float32
BF16 = jnp.bfloat16

D = 1152
TOK = 256
PATCH_VALS = 16
FREQ = 256
HEADS = 16
HEAD_DIM = 72
LATENT = 4096
GROUPS = 2
HALF = D // GROUPS
LANES = 128
CHUNK_ROWS = LATENT // LANES
PER_ROW = LANES // PATCH_VALS
FEATURE_TILES = D // LANES
ADA_TILES = 27
MOD_TILES = 45
CHIPS = 64

beta_low = 0.1
beta_high = 20.0
tol_abs = 0.0078
tol_rel = 0.05
norm_eps = 1e-06


def beta_at(moments):
    return beta_low + (beta_high - beta_low) * moments


def sigma_at(moments):
    integral = beta_low * moments + 0.5 * (beta_high - beta_low) * moments * moments
    return jnp.sqrt(1.0 - jnp.exp(-integral))


def lanes_of(shape):
    return lax.broadcasted_iota(jnp.int32, shape, len(shape) - 1)


def silu(values):
    return values / (1.0 + jnp.exp(-values))


def normed(values):
    average = jnp.sum(values, axis=-1, keepdims=True) * (1.0 / D)
    centred = values - average
    spread_sq = jnp.sum(centred * centred, axis=-1, keepdims=True) * (1.0 / D)
    return centred * lax.rsqrt(spread_sq + norm_eps)


def dot(a, b):
    return jnp.dot(a, b, preferred_element_type=F32)


def dot_t(a, b):
    return lax.dot_general(a, b, (((1,), (1,)), ((), ())), preferred_element_type=F32)


def peer_of(me, step):
    code = step + step // 42
    far_x, far_y, far_z = (code % 4 + 2) % 4, ((code // 4) % 4 + 2) % 4, (code // 16 + 2) % 4
    x, y, z = (me % 4 + far_x) % 4, ((me // 4) % 4 + far_y) % 4, (me // 16 + far_z) % 4
    return z * 16 + y * 4 + x


def kernel(
    now_ref,
    step_ref,
    accept_ref,
    current_ref,
    noise_ref,
    labels_ref,
    patch_ref,
    proj_ref,
    ada_ref,
    final_ref,
    time_in_ref,
    time_out_ref,
    qkv_ref,
    out_ref,
    state_ref,
    error_ref,
    time_in,
    time_out,
    wqkv,
    wout,
    stage,
    cond_send,
    cond_all,
    tiles_all,
    mod_send,
    mods,
    finals,
    patch8,
    proj8,
    table,
    stream,
    normal,
    qkv,
    mixed,
    rows,
    local_sem,
    tile_sem,
    swap_sem,
    cond_sem,
    weight_sem,
    mod_sem,
    final_sem,
):
    me = lax.axis_index("dp")
    side = lax.axis_index("tensor")
    other = 1 - side

    def at(chip, core):
        return {"dp": chip, "tensor": core}

    def own_row(pair):
        return jnp.where(side == 0, pair[0:1], pair[1:2])

    barrier = pltpu.get_barrier_semaphore()
    pl.semaphore_signal(barrier, inc=1, device_id=at(me, other), device_id_type=MESH)

    @pl.loop(0, CHIPS - 1)
    def _(step):
        pl.semaphore_signal(
            barrier, inc=1, device_id=at(peer_of(me, step), side), device_id_type=MESH
        )

    loads = [
        pltpu.make_async_copy(time_in_ref, time_in, local_sem.at[0]),
        pltpu.make_async_copy(time_out_ref, time_out, local_sem.at[1]),
        pltpu.make_async_copy(qkv_ref, wqkv.at[side], local_sem.at[2]),
        pltpu.make_async_copy(out_ref, wout.at[side], local_sem.at[3]),
    ]
    for copy in loads:
        copy.start()

    def put(tile, values):
        for pair in range(9):
            stage[side, tile, pair] = values[2 * pair : 2 * pair + 2]

    blank = jnp.zeros((18, 64), BF16)

    @pl.when(side == 0)
    def _():
        for tile in range(13):
            put(tile, ada_ref[0, :, tile * LANES : (tile + 1) * LANES])
        put(13, jnp.concatenate([ada_ref[0, :, 13 * LANES : 13 * LANES + 64], blank], axis=1))

    @pl.when(side == 1)
    def _():
        put(0, jnp.concatenate([blank, ada_ref[0, :, 0:64]], axis=1))
        for tile in range(1, 14):
            start = tile * LANES - 64
            put(tile, ada_ref[0, :, start : start + LANES])

    for tile in range(FEATURE_TILES):
        put(14 + tile, final_ref[:, tile * LANES : (tile + 1) * LANES])

    time_now = jnp.full((1, LANES), now_ref[side], F32)
    step_size = jnp.full((1, LANES), step_ref[side], F32)
    later = time_now - step_size
    moments = jnp.concatenate([time_now, later, jnp.zeros((6, LANES), F32)], axis=0)
    index = lanes_of((8, LANES)).astype(F32)
    rates = jnp.exp(-math.log(10000.0) * index / (FREQ // 2))
    angles = 1000.0 * moments * rates
    features = jnp.concatenate([jnp.cos(angles), jnp.sin(angles)], axis=1).astype(BF16)
    loads[0].wait()
    hidden = silu(dot(features, time_in[...])).astype(BF16)
    loads[1].wait()
    both = labels_ref[...].astype(F32)
    label = own_row(both)
    cond = silu(label + dot(hidden, time_out[...])).astype(BF16)
    for tile in range(FEATURE_TILES):
        piece = cond[0:2, tile * LANES : (tile + 1) * LANES]
        cond_send[tile] = piece
        cond_all[tile, me] = piece

    pl.semaphore_wait(barrier, CHIPS)

    tile_swap = pltpu.make_async_remote_copy(
        src_ref=stage.at[side],
        dst_ref=stage.at[side],
        send_sem=tile_sem.at[0],
        recv_sem=tile_sem.at[1],
        device_id=at(me, other),
        device_id_type=MESH,
    )
    tile_swap.start()

    @pl.loop(0, CHIPS - 1)
    def _(step):
        pltpu.make_async_remote_copy(
            src_ref=cond_send,
            dst_ref=cond_all.at[:, me],
            send_sem=cond_sem.at[0],
            recv_sem=cond_sem.at[1],
            device_id=at(peer_of(me, step), side),
            device_id_type=MESH,
        ).start()

    tile_swap.wait()
    for pair in range(9):
        stage[0, 13, pair] = stage[0, 13, pair] + stage[1, 0, pair]

    def send_tile(chip, core, tile):
        @pl.when(chip != me)
        def _():
            pltpu.make_async_remote_copy(
                src_ref=stage.at[core, tile],
                dst_ref=tiles_all.at[pl.ds(me * 9, 9)],
                send_sem=weight_sem.at[0],
                recv_sem=weight_sem.at[1],
                device_id=at(chip, side),
                device_id_type=MESH,
            ).start()

        @pl.when(chip == me)
        def _():
            tiles_all[pl.ds(me * 9, 9)] = stage[core, tile]

    @pl.loop(0, 14)
    def _(i):
        send_tile(i, 0, i)

    @pl.loop(14, 27)
    def _(i):
        send_tile(i, 1, i - 13)

    @pl.loop(27, 36)
    def _(i):
        send_tile(i, 0, i - 13)

    @pl.loop(36, 45)
    def _(i):
        send_tile(i, 1, i - 22)

    swaps = []
    for slot, (src, dst) in enumerate(((qkv_ref, wqkv), (out_ref, wout))):
        swaps.append(
            pltpu.make_async_remote_copy(
                src_ref=src,
                dst_ref=dst.at[side],
                send_sem=swap_sem.at[slot],
                recv_sem=swap_sem.at[2 + slot],
                device_id=at(me, other),
                device_id_type=MESH,
            )
        )
        swaps[-1].start()

    lane8 = lanes_of((CHUNK_ROWS, LANES)) // PATCH_VALS
    for piece in range(CHUNK_ROWS):
        span = slice(piece * LANES, (piece + 1) * LANES)
        rows[0, piece : piece + 1, :] = own_row(current_ref[:, span])
        rows[1, piece : piece + 1, :] = own_row(noise_ref[:, span])
    current = rows[0]
    draw = rows[1]
    for copy in range(PER_ROW):
        patch8[copy * PATCH_VALS : (copy + 1) * PATCH_VALS, :] = patch_ref[...]
    spread_lanes = (
        lax.broadcasted_iota(jnp.int32, (LANES, PATCH_VALS), 0) % PATCH_VALS
        == lanes_of((LANES, PATCH_VALS))
    )
    proj8[...] = dot(jnp.where(spread_lanes, 1.0, 0.0).astype(BF16), proj_ref[...]).astype(BF16)

    half = D // 2
    fill = jnp.zeros((TOK, 64), BF16)
    for group in range(GROUPS):
        for part in range(3):
            qkv[group, part, :, HALF:] = fill

    def table_chunk(j, carry):
        place = lax.broadcasted_iota(jnp.int32, (CHUNK_ROWS, D), 0) * PER_ROW + j
        column = lanes_of((CHUNK_ROWS, D))
        first = column < half
        freq = jnp.where(first, column, column - half).astype(F32)
        angle = place.astype(F32) * jnp.exp(-math.log(10000.0) * freq / half)
        table[pl.ds(pl.multiple_of(j * CHUNK_ROWS, CHUNK_ROWS), CHUNK_ROWS), :] = jnp.where(
            first, jnp.sin(angle), jnp.cos(angle)
        )
        return carry

    lax.fori_loop(0, PER_ROW, table_chunk, 0)

    def drain(ref, sem):
        pltpu.make_async_copy(ref, ref, sem).wait()

    drain(cond_all.at[:, pl.ds(0, CHIPS - 1)], cond_sem.at[1])

    @pl.when(me < MOD_TILES)
    def _():
        drain(tiles_all.at[pl.ds(0, 9 * (CHIPS - 1))], weight_sem.at[1])
        total = jnp.zeros((2 * CHIPS, LANES), F32)
        for tile in range(FEATURE_TILES):
            lhs = cond_all[tile].reshape(2 * CHIPS, LANES)
            rhs = tiles_all[tile * 64 : (tile + 1) * 64].reshape(LANES, LANES)
            total = total + dot(lhs, rhs)
        mod_send[...] = total.reshape(CHIPS, 2, LANES)
        mods[me] = mod_send[me]

        @pl.loop(0, CHIPS - 1)
        def _(step):
            chip = peer_of(me, step)
            pltpu.make_async_remote_copy(
                src_ref=mod_send.at[chip],
                dst_ref=mods.at[me],
                send_sem=mod_sem.at[0],
                recv_sem=mod_sem.at[1],
                device_id=at(chip, side),
                device_id_type=MESH,
            ).start()

    @pl.when(me < MOD_TILES)
    def _():
        drain(mods.at[pl.ds(0, MOD_TILES - 1)], mod_sem.at[1])

    @pl.when(me >= MOD_TILES)
    def _():
        drain(mods, mod_sem.at[1])

    loads[2].wait()
    loads[3].wait()
    for swap in swaps:
        swap.wait()

    def mod_row(which, moment):
        tiles = [mods[which * FEATURE_TILES + tile] for tile in range(FEATURE_TILES)]
        pair = jnp.concatenate(tiles, axis=1)
        return jnp.where(moment == 0, pair[0:1], pair[1:2])

    exponent = HEAD_DIM ** (-0.5) * math.log2(math.e)

    def evaluate(latent, moment):
        tokens = jnp.concatenate(
            [jnp.where(lane8 == j, latent, 0.0) for j in range(PER_ROW)], axis=0
        ).astype(BF16)
        stream[...] = dot(tokens, patch8[...]) + table[...]
        shift, scale = mod_row(0, moment), 1.0 + mod_row(1, moment)
        for j in range(PER_ROW):
            span = slice(j * CHUNK_ROWS, (j + 1) * CHUNK_ROWS)
            normal[span] = (normed(stream[span]) * scale + shift).astype(BF16)

        for group in range(GROUPS):
            for part in range(3):
                qkv[group, part, :, :HALF] = dot_t(normal[...], wqkv[group, part]).astype(BF16)

        def attend(group, carry):
            for head in range(HEADS // GROUPS):
                low, high = head * HEAD_DIM, (head + 1) * HEAD_DIM
                left = low // LANES * LANES
                right = -(-high // LANES) * LANES
                lane = lanes_of((1, right - left)) + left
                own = (lane >= low) & (lane < high)
                queries = qkv[group, 0, :, left:right]
                queries = jnp.where(own, queries, jnp.zeros_like(queries))
                scores = dot_t(queries, qkv[group, 1, :, left:right])
                top = jnp.max(scores, axis=-1, keepdims=True)
                weights = jnp.exp2((scores - top) * exponent)
                whole = jnp.sum(weights, axis=-1, keepdims=True)
                probs = (weights * (1.0 / whole)).astype(BF16)
                result = dot(probs, qkv[group, 2, :, left:right])
                for start in range(left, right, LANES):
                    piece = result[:, start - left : start - left + LANES]
                    if low > start:
                        past = lanes_of((1, LANES)) + start >= low
                        piece = jnp.where(past, piece, mixed[group, :, start : start + LANES].astype(F32))
                    mixed[group, :, start : start + LANES] = piece.astype(BF16)
            return carry

        lax.fori_loop(0, GROUPS, attend, 0)

        partial = [
            dot(mixed[group, :, :HALF], wout[group]).astype(BF16).astype(F32)
            for group in range(GROUPS)
        ]
        stream[...] = stream[...] + mod_row(2, moment) * (partial[0] + partial[1])
        shift, scale = mod_row(3, moment), 1.0 + mod_row(4, moment)
        for j in range(PER_ROW):
            span = slice(j * CHUNK_ROWS, (j + 1) * CHUNK_ROWS)
            normal[span] = (normed(stream[span]) * scale + shift).astype(BF16)
        guessed = dot_t(normal[...], proj8[...])
        result = jnp.zeros((CHUNK_ROWS, LANES), F32)
        for j in range(PER_ROW):
            result = result + jnp.where(
                lane8 == j, guessed[j * CHUNK_ROWS : (j + 1) * CHUNK_ROWS], 0.0
            )
        return result

    spread = jnp.sqrt(step_size * beta_at(time_now)) * draw

    rows[2] = current

    def one_moment(moment, carry):
        guess = evaluate(rows[2], moment)
        rows[4] = guess

        @pl.when(moment == 0)
        def _():
            rows[3] = guess
            beta = beta_at(time_now)
            drift_now = 0.5 * beta * rows[0] - beta * guess / sigma_at(time_now)
            rows[2] = rows[0] + step_size * drift_now + spread

        return carry

    lax.fori_loop(0, 2, one_moment, 0)

    current = rows[0]
    beta = beta_at(time_now)
    drift_now = 0.5 * beta * current - beta * rows[3] / sigma_at(time_now)
    euler = rows[2]
    beta_then = beta_at(later)
    drift_later = 0.5 * beta_then * euler - beta_then * rows[4] / sigma_at(later)
    heun = current + 0.5 * step_size * (drift_now + drift_later) + spread
    scale_ref = jnp.maximum(tol_abs, tol_rel * jnp.maximum(jnp.abs(heun), jnp.abs(current)))
    gap = (euler - heun) / scale_ref
    squares = jnp.sum(jnp.sum(gap * gap, axis=1, keepdims=True), axis=0, keepdims=True)
    error = jnp.sqrt(squares / LATENT)
    taken = jnp.full((CHUNK_ROWS, LANES), accept_ref[side], jnp.int32) == 1
    finals[side, :CHUNK_ROWS] = jnp.where(taken, heun, current)
    finals[side, CHUNK_ROWS:] = jnp.broadcast_to(error, (8, LANES))
    final_swap = pltpu.make_async_remote_copy(
        src_ref=finals.at[side],
        dst_ref=finals.at[side],
        send_sem=final_sem.at[0],
        recv_sem=final_sem.at[1],
        device_id=at(me, other),
        device_id_type=MESH,
    )
    final_swap.start()

    drain(cond_all.at[:, pl.ds(0, CHIPS - 1)], cond_sem.at[0])
    @pl.when(me >= MOD_TILES)
    def _():
        drain(tiles_all.at[pl.ds(0, 9 * MOD_TILES)], weight_sem.at[0])

    @pl.when(me < MOD_TILES)
    def _():
        drain(tiles_all.at[pl.ds(0, 9 * (MOD_TILES - 1))], weight_sem.at[0])
        drain(mod_send.at[pl.ds(0, CHIPS - 1)], mod_sem.at[0])

    final_swap.wait()
    for latent in range(2):
        for piece in range(CHUNK_ROWS):
            state_ref[latent : latent + 1, piece * LANES : (piece + 1) * LANES] = finals[
                latent, piece : piece + 1, :
            ]
        error_ref[latent : latent + 1, :] = finals[latent, CHUNK_ROWS : CHUNK_ROWS + 1, :]


def shards(
    current,
    noise_draw,
    labels,
    time_now,
    step_size,
    accept,
    patch_weight,
    time_in,
    time_out,
    qkv_weight,
    out_weight,
    ada_weight,
    final_ada,
    final_proj,
):
    smem = pl.BlockSpec(memory_space=pltpu.SMEM)
    vmem = pl.BlockSpec(memory_space=pltpu.VMEM)
    place = pl.BlockSpec(memory_space=pl.ANY)
    state, error = pl.pallas_call(
        kernel,
        out_shape=(
            jax.ShapeDtypeStruct((2, LATENT), F32),
            jax.ShapeDtypeStruct((2, LANES), F32),
        ),
        in_specs=[smem] * 3 + [vmem] * 7 + [place] * 4,
        out_specs=(vmem, vmem),
        scratch_shapes=[
            pltpu.VMEM((FREQ, D), BF16),
            pltpu.VMEM((D, D), BF16),
            pltpu.VMEM((GROUPS, 3, HALF, D), BF16),
            pltpu.VMEM((GROUPS, HALF, D), BF16),
            pltpu.VMEM((2, 23, 9, 2, LANES), BF16),
            pltpu.VMEM((FEATURE_TILES, 2, LANES), BF16),
            pltpu.VMEM((FEATURE_TILES, CHIPS, 2, LANES), BF16),
            pltpu.VMEM((9 * CHIPS, 2, LANES), BF16),
            pltpu.VMEM((CHIPS, 2, LANES), F32),
            pltpu.VMEM((MOD_TILES, 2, LANES), F32),
            pltpu.VMEM((2, CHUNK_ROWS + 8, LANES), F32),
            pltpu.VMEM((LANES, D), BF16),
            pltpu.VMEM((LANES, D), BF16),
            pltpu.VMEM((TOK, D), F32),
            pltpu.VMEM((TOK, D), F32),
            pltpu.VMEM((TOK, D), BF16),
            pltpu.VMEM((GROUPS, 3, TOK, 640), BF16),
            pltpu.VMEM((GROUPS, TOK, 640), BF16),
            pltpu.VMEM((5, CHUNK_ROWS, LANES), F32),
            pltpu.SemaphoreType.DMA((4,)),
            pltpu.SemaphoreType.DMA((2,)),
            pltpu.SemaphoreType.DMA((4,)),
            pltpu.SemaphoreType.DMA((2,)),
            pltpu.SemaphoreType.DMA((2,)),
            pltpu.SemaphoreType.DMA((2,)),
            pltpu.SemaphoreType.DMA((2,)),
        ],
        compiler_params=pltpu.CompilerParams(
            collective_id=0, has_side_effects=True, vmem_limit_bytes=60 * 1024 * 1024
        ),
        name="heun_step",
    )(
        time_now,
        step_size,
        accept,
        current,
        noise_draw,
        labels,
        patch_weight,
        final_proj.T,
        ada_weight,
        final_ada,
        time_in,
        time_out,
        qkv_weight[0].transpose(1, 2, 0),
        out_weight[0].T,
    )
    return state, error[:, 0]


def solution(mesh):
    in_specs = (
        P("dp", None),
        P("dp", None),
        P("dp", None),
        P("dp"),
        P("dp"),
        P("dp"),
        P(),
        P(),
        P(),
        P(None, None, None, "tensor"),
        P(None, None, "tensor"),
        P(None, "dp", "tensor"),
        P("dp", "tensor"),
        P(),
    )
    out_specs = (P("dp", None), P("dp"))
    return jax.shard_map(shards, mesh=mesh, in_specs=in_specs, out_specs=out_specs, check_vma=False)
```

```python
import functools
import math

import jax
import jax.numpy as jnp
from jax import lax
from jax.experimental import pallas as pl
from jax.experimental.pallas import tpu as pltpu
from jax.sharding import PartitionSpec as P

MESH = pl.DeviceIdType.MESH
F32 = jnp.float32
BF16 = jnp.bfloat16

D = 1152
TOK = 256
PATCH_VALS = 16
FREQ = 256
HEADS = 16
HEAD_DIM = 72
LATENT = 4096
GROUPS = 2
HALF = D // GROUPS
LANES = 128
CHUNK_ROWS = LATENT // LANES
PER_ROW = LANES // PATCH_VALS
FEATURE_TILES = D // LANES
MOD_TILES = 45
CHIPS = 64
TILE_CHIPS = (
    tuple(range(9)),
    (9, 10, 11, 12, 13, 23, 24, 25, 26),
    tuple(range(27, 36)),
    tuple(range(14, 23)),
    tuple(range(36, 45)),
)

beta_low = 0.1
beta_high = 20.0
tol_abs = 0.0078
tol_rel = 0.05
norm_eps = 1e-06


def beta_at(moments):
    return beta_low + (beta_high - beta_low) * moments


def sigma_at(moments):
    integral = beta_low * moments + 0.5 * (beta_high - beta_low) * moments * moments
    return jnp.sqrt(1.0 - jnp.exp(-integral))


def lanes_of(shape):
    return lax.broadcasted_iota(jnp.int32, shape, len(shape) - 1)


def silu(values):
    return values / (1.0 + jnp.exp(-values))


def normed(values):
    average = jnp.sum(values, axis=-1, keepdims=True) * (1.0 / D)
    centred = values - average
    spread_sq = jnp.sum(centred * centred, axis=-1, keepdims=True) * (1.0 / D)
    return centred * lax.rsqrt(spread_sq + norm_eps)


def dot(a, b):
    return jnp.dot(a, b, preferred_element_type=F32)


def dot_t(a, b):
    return lax.dot_general(a, b, (((1,), (1,)), ((), ())), preferred_element_type=F32)


OFFSETS = sorted(
    ((z, y, x) for z in (2, 1, 3, 0) for y in (2, 1, 3, 0) for x in (2, 1, 3, 0) if z + y + x),
    key=lambda offset: -sum(min(step, 4 - step) for step in offset),
)


def kernel(
    now_ref,
    step_ref,
    accept_ref,
    current_ref,
    noise_ref,
    labels_ref,
    patch_ref,
    proj_ref,
    ada_ref,
    final_ref,
    time_in_ref,
    time_out_ref,
    qkv_ref,
    out_ref,
    state_ref,
    error_ref,
    time_in,
    time_out,
    wqkv,
    wout,
    stage,
    cond_send,
    cond_all,
    tiles_all,
    mod_send,
    mods,
    finals,
    patch8,
    proj8,
    table,
    stream,
    normal,
    queries,
    keys,
    values,
    mixed,
    turned,
    scores,
    probs,
    rows,
    local_sem,
    tile_sem,
    swap_sem,
    cond_sem,
    weight_sem,
    mod_sem,
    final_sem,
):
    me = lax.axis_index("dp")
    side = lax.axis_index("tensor")
    other = 1 - side

    def at(chip, core):
        return {"dp": chip, "tensor": core}

    def own_row(pair):
        return jnp.where(side == 0, pair[0:1], pair[1:2])

    barrier = pltpu.get_barrier_semaphore()
    pl.semaphore_signal(barrier, inc=1, device_id=at(me, other), device_id_type=MESH)

    along_x = [lax.rem(me + step, 4) for step in range(4)]
    along_y = [lax.rem(me // 4 + step, 4) * 4 for step in range(4)]
    along_z = [lax.rem(me // 16 + step, 4) * 16 for step in range(4)]
    peers = [along_z[z] + along_y[y] + along_x[x] for z, y, x in OFFSETS]
    for chip in peers:
        pl.semaphore_signal(barrier, inc=1, device_id=at(chip, side), device_id_type=MESH)

    loads = [
        pltpu.make_async_copy(time_in_ref, time_in, local_sem.at[0]),
        pltpu.make_async_copy(time_out_ref, time_out, local_sem.at[1]),
        pltpu.make_async_copy(qkv_ref, wqkv.at[:, side], local_sem.at[2]),
        pltpu.make_async_copy(out_ref, wout.at[side], local_sem.at[3]),
    ]
    for copy in loads:
        copy.start()

    def put(tile, values):
        for pair in range(9):
            stage[tile, pair] = values[2 * pair : 2 * pair + 2]

    blank = jnp.zeros((18, 64), BF16)

    @pl.when(side == 0)
    def _():
        for tile in range(13):
            put(tile, ada_ref[0, :, tile * LANES : (tile + 1) * LANES])
        for tile in range(FEATURE_TILES):
            put(14 + tile, final_ref[:, tile * LANES : (tile + 1) * LANES])
        put(13, jnp.concatenate([ada_ref[0, :, 13 * LANES : 13 * LANES + 64], blank], axis=1))

    @pl.when(side == 1)
    def _():
        put(MOD_TILES, jnp.concatenate([blank, ada_ref[0, :, 0:64]], axis=1))
        for tile in range(1, 14):
            start = tile * LANES - 64
            put(22 + tile, ada_ref[0, :, start : start + LANES])
        for tile in range(FEATURE_TILES):
            put(36 + tile, final_ref[:, tile * LANES : (tile + 1) * LANES])

    time_now = jnp.full((1, LANES), now_ref[side], F32)
    step_size = jnp.full((1, LANES), step_ref[side], F32)
    later = time_now - step_size
    moments = jnp.concatenate([time_now, later, jnp.zeros((6, LANES), F32)], axis=0)
    index = lanes_of((8, LANES)).astype(F32)
    rates = jnp.exp(-math.log(10000.0) * index / (FREQ // 2))
    angles = 1000.0 * moments * rates
    features = jnp.concatenate([jnp.cos(angles), jnp.sin(angles)], axis=1).astype(BF16)
    loads[0].wait()
    hidden = silu(dot(features, time_in[...])).astype(BF16)
    loads[1].wait()
    both = labels_ref[...].astype(F32)
    label = own_row(both)
    cond = silu(label + dot(hidden, time_out[...])).astype(BF16)
    for tile in range(FEATURE_TILES):
        piece = cond[0:2, tile * LANES : (tile + 1) * LANES]
        cond_send[tile] = piece
        cond_all[tile, me] = piece

    pl.semaphore_wait(barrier, CHIPS)

    tile_swap = pltpu.make_async_remote_copy(
        src_ref=stage.at[pl.ds(side * 23, 23)],
        dst_ref=stage.at[pl.ds(side * 23, 23)],
        send_sem=tile_sem.at[0],
        recv_sem=tile_sem.at[1],
        device_id=at(me, other),
        device_id_type=MESH,
    )
    tile_swap.start()

    for chip in peers:
        pltpu.make_async_remote_copy(
            src_ref=cond_send,
            dst_ref=cond_all.at[:, me],
            send_sem=cond_sem.at[0],
            recv_sem=cond_sem.at[1],
            device_id=at(chip, side),
            device_id_type=MESH,
        ).start()

    tile_swap.wait()
    for pair in range(9):
        stage[13, pair] = stage[13, pair] + stage[MOD_TILES, pair]

    for chip in peers:

        @pl.when(chip < MOD_TILES)
        def _():
            pltpu.make_async_remote_copy(
                src_ref=stage.at[chip],
                dst_ref=tiles_all.at[pl.ds(me * 9, 9)],
                send_sem=weight_sem.at[0],
                recv_sem=weight_sem.at[1],
                device_id=at(chip, side),
                device_id_type=MESH,
            ).start()

    @pl.when(me < MOD_TILES)
    def _():
        tiles_all[pl.ds(me * 9, 9)] = stage[me]

    swaps = []
    for slot, (src, dst) in enumerate(((qkv_ref, wqkv.at[:, side]), (out_ref, wout.at[side]))):
        swaps.append(
            pltpu.make_async_remote_copy(
                src_ref=src,
                dst_ref=dst,
                send_sem=swap_sem.at[slot],
                recv_sem=swap_sem.at[2 + slot],
                device_id=at(me, other),
                device_id_type=MESH,
            )
        )
        swaps[-1].start()

    lane8 = lanes_of((CHUNK_ROWS, LANES)) // PATCH_VALS
    for piece in range(CHUNK_ROWS):
        span = slice(piece * LANES, (piece + 1) * LANES)
        rows[0, piece : piece + 1, :] = own_row(current_ref[:, span])
        rows[1, piece : piece + 1, :] = own_row(noise_ref[:, span])
    current = rows[0]
    draw = rows[1]
    for copy in range(PER_ROW):
        patch8[copy * PATCH_VALS : (copy + 1) * PATCH_VALS, :] = patch_ref[...]
    spread_lanes = (
        lax.broadcasted_iota(jnp.int32, (LANES, PATCH_VALS), 0) % PATCH_VALS
        == lanes_of((LANES, PATCH_VALS))
    )
    proj8[...] = dot(jnp.where(spread_lanes, 1.0, 0.0).astype(BF16), proj_ref[...]).astype(BF16)

    half = D // 2
    def table_chunk(j, carry):
        place = lax.broadcasted_iota(jnp.int32, (CHUNK_ROWS, D), 0) * PER_ROW + j
        column = lanes_of((CHUNK_ROWS, D))
        first = column < half
        freq = jnp.where(first, column, column - half).astype(F32)
        angle = place.astype(F32) * jnp.exp(-math.log(10000.0) * freq / half)
        table[pl.ds(pl.multiple_of(j * CHUNK_ROWS, CHUNK_ROWS), CHUNK_ROWS), :] = jnp.where(
            first, jnp.sin(angle), jnp.cos(angle)
        )
        return carry

    lax.fori_loop(0, PER_ROW, table_chunk, 0)

    def drain(ref, sem):
        pltpu.make_async_copy(ref, ref, sem).wait()

    drain(cond_all.at[:, pl.ds(0, CHIPS - 1)], cond_sem.at[1])

    @pl.when(me < MOD_TILES)
    def _():
        drain(tiles_all.at[pl.ds(0, 9 * (CHIPS - 1))], weight_sem.at[1])
        total = jnp.zeros((2 * CHIPS, LANES), F32)
        for tile in range(FEATURE_TILES):
            lhs = cond_all[tile].reshape(2 * CHIPS, LANES)
            rhs = tiles_all[tile * 64 : (tile + 1) * 64].reshape(LANES, LANES)
            total = total + dot(lhs, rhs)
        mod_send[...] = total.reshape(CHIPS, 2, LANES)
        mods[me] = mod_send[me]

        for chip in peers:
            pltpu.make_async_remote_copy(
                src_ref=mod_send.at[chip],
                dst_ref=mods.at[me],
                send_sem=mod_sem.at[0],
                recv_sem=mod_sem.at[1],
                device_id=at(chip, side),
                device_id_type=MESH,
            ).start()

    @pl.when(me < MOD_TILES)
    def _():
        drain(mods.at[pl.ds(0, MOD_TILES - 1)], mod_sem.at[1])

    @pl.when(me >= MOD_TILES)
    def _():
        drain(mods, mod_sem.at[1])

    loads[2].wait()
    loads[3].wait()
    for swap in swaps:
        swap.wait()

    def mod_row(which, moment):
        tiles = [mods[chip] for chip in TILE_CHIPS[which]]
        pair = jnp.concatenate(tiles, axis=1)
        return jnp.where(moment == 0, pair[0:1], pair[1:2])

    exponent = HEAD_DIM ** (-0.5) * math.log2(math.e)

    def evaluate(latent, moment):
        tokens = jnp.concatenate(
            [jnp.where(lane8 == j, latent, 0.0) for j in range(PER_ROW)], axis=0
        ).astype(BF16)
        stream[...] = dot(tokens, patch8[...]) + table[...]
        shift, scale = mod_row(0, moment), 1.0 + mod_row(1, moment)
        for j in range(PER_ROW):
            span = slice(j * CHUNK_ROWS, (j + 1) * CHUNK_ROWS)
            normal[span] = (normed(stream[span]) * scale + shift).astype(BF16)

        turned[...] = normal[...].T
        weight = [wqkv[part].reshape(D, D) for part in range(3)]
        queries[...] = (dot(weight[0], turned[...]) * exponent).astype(BF16)
        keys[...] = dot(weight[1], turned[...]).astype(BF16).T
        values[...] = dot(weight[2], turned[...]).astype(BF16)

        def score(head):
            low, high = head * HEAD_DIM, (head + 1) * HEAD_DIM
            left = low // LANES * LANES
            right = -(-high // LANES) * LANES
            row = lax.broadcasted_iota(jnp.int32, (right - left, 1), 0) + left
            asked = queries[left:right]
            asked = jnp.where((row >= low) & (row < high), asked, jnp.zeros_like(asked))
            scores[head % 2] = dot(keys[:, left:right], asked)

        def soften(head):
            found = scores[head % 2]
            weights = jnp.exp2(found - jnp.max(found, axis=0, keepdims=True))
            probs[head % 2] = weights.astype(BF16)
            return jnp.sum(weights, axis=0, keepdims=True)

        def apply(head, whole):
            low, high = head * HEAD_DIM, (head + 1) * HEAD_DIM
            first = low // 16 * 16
            result = dot(values[first : first + 80], probs[head % 2])
            mixed[low:high] = result[low - first : high - first] * (1.0 / whole)

        score(0)
        before = None
        for head in range(HEADS):
            if head + 1 < HEADS:
                score(head + 1)
            whole = soften(head)
            if head:
                apply(head - 1, before)
            before = whole
        apply(HEADS - 1, before)

        attended = lax.dot_general(
            mixed[...].astype(BF16),
            wout[...].reshape(D, D),
            (((0,), (0,)), ((), ())),
            preferred_element_type=F32,
        )
        stream[...] = stream[...] + mod_row(2, moment) * attended
        shift, scale = mod_row(3, moment), 1.0 + mod_row(4, moment)
        for j in range(PER_ROW):
            span = slice(j * CHUNK_ROWS, (j + 1) * CHUNK_ROWS)
            normal[span] = (normed(stream[span]) * scale + shift).astype(BF16)
        guessed = dot_t(normal[...], proj8[...])
        result = jnp.zeros((CHUNK_ROWS, LANES), F32)
        for j in range(PER_ROW):
            result = result + jnp.where(
                lane8 == j, guessed[j * CHUNK_ROWS : (j + 1) * CHUNK_ROWS], 0.0
            )
        return result

    spread = jnp.sqrt(step_size * beta_at(time_now)) * draw

    rows[2] = current

    def one_moment(moment, carry):
        guess = evaluate(rows[2], moment)
        rows[4] = guess

        @pl.when(moment == 0)
        def _():
            rows[3] = guess
            beta = beta_at(time_now)
            drift_now = 0.5 * beta * rows[0] - beta * guess / sigma_at(time_now)
            rows[2] = rows[0] + step_size * drift_now + spread

        return carry

    lax.fori_loop(0, 2, one_moment, 0)

    current = rows[0]
    beta = beta_at(time_now)
    drift_now = 0.5 * beta * current - beta * rows[3] / sigma_at(time_now)
    euler = rows[2]
    beta_then = beta_at(later)
    drift_later = 0.5 * beta_then * euler - beta_then * rows[4] / sigma_at(later)
    heun = current + 0.5 * step_size * (drift_now + drift_later) + spread
    scale_ref = jnp.maximum(tol_abs, tol_rel * jnp.maximum(jnp.abs(heun), jnp.abs(current)))
    gap = (euler - heun) / scale_ref
    squares = jnp.sum(jnp.sum(gap * gap, axis=1, keepdims=True), axis=0, keepdims=True)
    error = jnp.sqrt(squares / LATENT)
    taken = jnp.full((CHUNK_ROWS, LANES), accept_ref[side], jnp.int32) == 1
    finals[side, :CHUNK_ROWS] = jnp.where(taken, heun, current)
    finals[side, CHUNK_ROWS:] = jnp.broadcast_to(error, (8, LANES))
    final_swap = pltpu.make_async_remote_copy(
        src_ref=finals.at[side],
        dst_ref=finals.at[side],
        send_sem=final_sem.at[0],
        recv_sem=final_sem.at[1],
        device_id=at(me, other),
        device_id_type=MESH,
    )
    final_swap.start()

    drain(cond_all.at[:, pl.ds(0, CHIPS - 1)], cond_sem.at[0])
    @pl.when(me >= MOD_TILES)
    def _():
        drain(tiles_all.at[pl.ds(0, 9 * MOD_TILES)], weight_sem.at[0])

    @pl.when(me < MOD_TILES)
    def _():
        drain(tiles_all.at[pl.ds(0, 9 * (MOD_TILES - 1))], weight_sem.at[0])
        drain(mod_send.at[pl.ds(0, CHIPS - 1)], mod_sem.at[0])

    final_swap.wait()
    for latent in range(2):
        for piece in range(CHUNK_ROWS):
            state_ref[latent : latent + 1, piece * LANES : (piece + 1) * LANES] = finals[
                latent, piece : piece + 1, :
            ]
        error_ref[latent : latent + 1, :] = finals[latent, CHUNK_ROWS : CHUNK_ROWS + 1, :]


def shards(
    current,
    noise_draw,
    labels,
    time_now,
    step_size,
    accept,
    patch_weight,
    time_in,
    time_out,
    qkv_weight,
    out_weight,
    ada_weight,
    final_ada,
    final_proj,
):
    smem = pl.BlockSpec(memory_space=pltpu.SMEM)
    vmem = pl.BlockSpec(memory_space=pltpu.VMEM)
    place = pl.BlockSpec(memory_space=pl.ANY)
    state, error = pl.pallas_call(
        kernel,
        out_shape=(
            jax.ShapeDtypeStruct((2, LATENT), F32),
            jax.ShapeDtypeStruct((2, LANES), F32),
        ),
        in_specs=[smem] * 3 + [vmem] * 7 + [place] * 4,
        out_specs=(vmem, vmem),
        scratch_shapes=[
            pltpu.VMEM((FREQ, D), BF16),
            pltpu.VMEM((D, D), BF16),
            pltpu.VMEM((3, GROUPS, HALF, D), BF16),
            pltpu.VMEM((GROUPS, HALF, D), BF16),
            pltpu.VMEM((MOD_TILES + 1, 9, 2, LANES), BF16),
            pltpu.VMEM((FEATURE_TILES, 2, LANES), BF16),
            pltpu.VMEM((FEATURE_TILES, CHIPS, 2, LANES), BF16),
            pltpu.VMEM((9 * CHIPS, 2, LANES), BF16),
            pltpu.VMEM((CHIPS, 2, LANES), F32),
            pltpu.VMEM((MOD_TILES, 2, LANES), F32),
            pltpu.VMEM((2, CHUNK_ROWS + 8, LANES), F32),
            pltpu.VMEM((LANES, D), BF16),
            pltpu.VMEM((LANES, D), BF16),
            pltpu.VMEM((TOK, D), F32),
            pltpu.VMEM((TOK, D), F32),
            pltpu.VMEM((TOK, D), BF16),
            pltpu.VMEM((D, TOK), BF16),
            pltpu.VMEM((TOK, D), BF16),
            pltpu.VMEM((D, TOK), BF16),
            pltpu.VMEM((D, TOK), F32),
            pltpu.VMEM((D, TOK), BF16),
            pltpu.VMEM((2, TOK, TOK), F32),
            pltpu.VMEM((2, TOK, TOK), BF16),
            pltpu.VMEM((5, CHUNK_ROWS, LANES), F32),
            pltpu.SemaphoreType.DMA((4,)),
            pltpu.SemaphoreType.DMA((2,)),
            pltpu.SemaphoreType.DMA((4,)),
            pltpu.SemaphoreType.DMA((2,)),
            pltpu.SemaphoreType.DMA((2,)),
            pltpu.SemaphoreType.DMA((2,)),
            pltpu.SemaphoreType.DMA((2,)),
        ],
        compiler_params=pltpu.CompilerParams(
            collective_id=0, has_side_effects=True, vmem_limit_bytes=60 * 1024 * 1024
        ),
        name="heun_step",
    )(
        time_now,
        step_size,
        accept,
        current,
        noise_draw,
        labels,
        patch_weight,
        final_proj.T,
        ada_weight,
        final_ada,
        time_in,
        time_out,
        qkv_weight[0].transpose(1, 2, 0),
        out_weight[0].T,
    )
    return state, error[:, 0]


def solution(mesh):
    in_specs = (
        P("dp", None),
        P("dp", None),
        P("dp", None),
        P("dp"),
        P("dp"),
        P("dp"),
        P(),
        P(),
        P(),
        P(None, None, None, "tensor"),
        P(None, None, "tensor"),
        P(None, "dp", "tensor"),
        P("dp", "tensor"),
        P(),
    )
    out_specs = (P("dp", None), P("dp"))
    return jax.shard_map(shards, mesh=mesh, in_specs=in_specs, out_specs=out_specs, check_vma=False)
```

```python
import functools
import math

import jax
import jax.numpy as jnp
from jax import lax
from jax.experimental import pallas as pl
from jax.experimental.pallas import tpu as pltpu
from jax.sharding import PartitionSpec as P

MESH = pl.DeviceIdType.MESH
F32 = jnp.float32
BF16 = jnp.bfloat16

D = 1152
TOK = 256
PATCH_VALS = 16
FREQ = 256
HEADS = 16
HEAD_DIM = 72
LATENT = 4096
GROUPS = 2
HALF = D // GROUPS
LANES = 128
CHUNK_ROWS = LATENT // LANES
PER_ROW = LANES // PATCH_VALS
FEATURE_TILES = D // LANES
MOD_TILES = 46
SIDE_TILES = 23
CHIPS = 64
TILE_CHIPS = (
    tuple(range(9)),
    (9, 10, 11, 12, 13, 23, 24, 25, 26),
    tuple(range(27, 36)),
    tuple(range(14, 23)),
    tuple(range(36, 45)),
)

beta_low = 0.1
beta_high = 20.0
tol_abs = 0.0078
tol_rel = 0.05
norm_eps = 1e-06


def beta_at(moments):
    return beta_low + (beta_high - beta_low) * moments


def sigma_at(moments):
    integral = beta_low * moments + 0.5 * (beta_high - beta_low) * moments * moments
    return jnp.sqrt(1.0 - jnp.exp(-integral))


def lanes_of(shape):
    return lax.broadcasted_iota(jnp.int32, shape, len(shape) - 1)


def silu(values):
    return values / (1.0 + jnp.exp(-values))


def moments_of(ref, spans):
    means = [jnp.sum(ref[span], axis=-1, keepdims=True) * (1.0 / D) for span in spans]
    spreads = []
    for span, mean in zip(spans, means):
        centred = ref[span] - mean
        spread_sq = jnp.sum(centred * centred, axis=-1, keepdims=True) * (1.0 / D)
        spreads.append(lax.rsqrt(spread_sq + norm_eps))
    return means, spreads


def dot(a, b):
    return jnp.dot(a, b, preferred_element_type=F32)


def dot_t(a, b):
    return lax.dot_general(a, b, (((1,), (1,)), ((), ())), preferred_element_type=F32)


OFFSETS = sorted(
    ((z, y, x) for z in (2, 1, 3, 0) for y in (2, 1, 3, 0) for x in (2, 1, 3, 0) if z + y + x),
    key=lambda offset: -sum(min(step, 4 - step) for step in offset),
)


def kernel(
    now_in,
    step_in,
    accept_in,
    current_in,
    noise_in,
    labels_in,
    patch_in,
    proj_in,
    ada_in,
    final_in,
    time_in_ref,
    time_out_ref,
    qkv_ref,
    out_ref,
    state_ref,
    error_ref,
    now_ref,
    step_ref,
    accept_ref,
    current_ref,
    noise_ref,
    labels_ref,
    patch_ref,
    proj_ref,
    ada_ref,
    final_ref,
    time_in,
    time_out,
    wqkv,
    wout,
    stage,
    cond_send,
    cond_all,
    tiles_all,
    mod_send,
    mods,
    finals,
    patch8,
    proj8,
    table,
    unit,
    stream,
    normal,
    queries,
    keys,
    values,
    mixed,
    turned,
    scores,
    probs,
    rows,
    local_sem,
    small_sem,
    tile_sem,
    swap_sem,
    cond_sem,
    weight_sem,
    mod_sem,
    final_sem,
):
    me = lax.axis_index("dp")
    side = lax.axis_index("tensor")
    other = 1 - side

    def at(chip, core):
        return {"dp": chip, "tensor": core}

    def own_row(pair):
        return jnp.where(side == 0, pair[0:1], pair[1:2])

    loads = [
        pltpu.make_async_copy(time_in_ref, time_in, local_sem.at[0]),
        pltpu.make_async_copy(time_out_ref, time_out, local_sem.at[1]),
        pltpu.make_async_copy(qkv_ref, wqkv.at[:, side], local_sem.at[2]),
        pltpu.make_async_copy(out_ref, wout.at[side], local_sem.at[3]),
    ]
    for copy in loads[:2]:
        copy.start()
    small = [
        pltpu.make_async_copy(source, target, small_sem.at[slot])
        for slot, (source, target) in enumerate(
            (
                (now_in, now_ref),
                (step_in, step_ref),
                (ada_in, ada_ref),
                (final_in, final_ref),
                (labels_in, labels_ref),
                (current_in, current_ref),
                (noise_in, noise_ref),
                (patch_in, patch_ref),
                (proj_in, proj_ref),
                (accept_in, accept_ref),
            )
        )
    ]
    for copy in small:
        copy.start()

    barrier = pltpu.get_barrier_semaphore()
    pl.semaphore_signal(barrier, inc=1, device_id=at(me, other), device_id_type=MESH)

    along_x = [lax.rem(me + step, 4) for step in range(4)]
    along_y = [lax.rem(me // 4 + step, 4) * 4 for step in range(4)]
    along_z = [lax.rem(me // 16 + step, 4) * 16 for step in range(4)]
    peers = [along_z[z] + along_y[y] + along_x[x] for z, y, x in OFFSETS]
    holder = me < MOD_TILES

    @pl.when(holder)
    def _():
        for chip in peers:
            pl.semaphore_signal(barrier, inc=1, device_id=at(chip, side), device_id_type=MESH)

    small[2].wait()
    small[3].wait()

    def put(tile, values):
        for pair in range(9):
            stage[tile, pair] = values[2 * pair : 2 * pair + 2]

    blank = jnp.zeros((18, 64), BF16)

    @pl.when(side == 0)
    def _():
        for tile in range(13):
            put(tile, ada_ref[0, :, tile * LANES : (tile + 1) * LANES])
        for tile in range(FEATURE_TILES):
            put(14 + tile, final_ref[:, tile * LANES : (tile + 1) * LANES])
        put(13, jnp.concatenate([ada_ref[0, :, 13 * LANES : 13 * LANES + 64], blank], axis=1))

    @pl.when(side == 1)
    def _():
        put(MOD_TILES - 1, jnp.concatenate([blank, ada_ref[0, :, 0:64]], axis=1))
        for tile in range(1, 14):
            start = tile * LANES - 64
            put(22 + tile, ada_ref[0, :, start : start + LANES])
        for tile in range(FEATURE_TILES):
            put(36 + tile, final_ref[:, tile * LANES : (tile + 1) * LANES])

    for slot in (0, 1, 4):
        small[slot].wait()
    time_now = jnp.full((1, LANES), now_ref[side], F32)
    step_size = jnp.full((1, LANES), step_ref[side], F32)
    later = time_now - step_size
    moments = jnp.concatenate([time_now, later, jnp.zeros((6, LANES), F32)], axis=0)

    def condition():
        index = lanes_of((8, LANES)).astype(F32)
        rates = jnp.exp(-math.log(10000.0) * index / (FREQ // 2))
        angles = 1000.0 * moments * rates
        features = jnp.concatenate([jnp.cos(angles), jnp.sin(angles)], axis=1).astype(BF16)
        loads[0].wait()
        hidden = silu(dot(features, time_in[...])).astype(BF16)
        loads[1].wait()
        loads[2].start()
        loads[3].start()
        label = own_row(labels_ref[...].astype(F32))
        cond = silu(label + dot(hidden, time_out[...])).astype(BF16)
        for tile in range(FEATURE_TILES):
            piece = cond[0:2, tile * LANES : (tile + 1) * LANES]
            cond_send[tile] = piece
            cond_all[tile, me] = piece

    early = me < CHIPS // 2
    pl.when(early)(condition)

    @pl.when(holder)
    def _():
        pl.semaphore_wait(barrier, MOD_TILES)

    @pl.when(jnp.logical_not(holder))
    def _():
        pl.semaphore_wait(barrier, MOD_TILES + 1)

    pl.when(jnp.logical_not(early))(condition)

    for chip in peers:

        @pl.when(chip < MOD_TILES)
        def _():
            pltpu.make_async_remote_copy(
                src_ref=cond_send,
                dst_ref=cond_all.at[:, me],
                send_sem=cond_sem.at[0],
                recv_sem=cond_sem.at[1],
                device_id=at(chip, side),
                device_id_type=MESH,
            ).start()

    def ours(chip):
        return jnp.logical_and(chip < MOD_TILES, (chip < SIDE_TILES) == (side == 0))

    direct = ours(me)
    for chip in peers:

        @pl.when(ours(chip))
        def _():
            pltpu.make_async_remote_copy(
                src_ref=stage.at[chip],
                dst_ref=tiles_all.at[pl.ds(me * 9, 9)],
                send_sem=weight_sem.at[0],
                recv_sem=weight_sem.at[1],
                device_id=at(chip, side),
                device_id_type=MESH,
            ).start()

    @pl.when(direct)
    def _():
        tiles_all[pl.ds(me * 9, 9)] = stage[me]

    tile_share = pltpu.make_async_remote_copy(
        src_ref=tiles_all,
        dst_ref=tiles_all,
        send_sem=tile_sem.at[0],
        recv_sem=tile_sem.at[1],
        device_id=at(me, other),
        device_id_type=MESH,
    )

    swaps = []
    for slot, (src, dst) in enumerate(((qkv_ref, wqkv.at[:, side]), (out_ref, wout.at[side]))):
        swaps.append(
            pltpu.make_async_remote_copy(
                src_ref=src,
                dst_ref=dst,
                send_sem=swap_sem.at[slot],
                recv_sem=swap_sem.at[2 + slot],
                device_id=at(me, other),
                device_id_type=MESH,
            )
        )
        swaps[-1].start()

    for copy in small[5:]:
        copy.wait()
    lane8 = lanes_of((CHUNK_ROWS, LANES)) // PATCH_VALS
    for piece in range(CHUNK_ROWS):
        span = slice(piece * LANES, (piece + 1) * LANES)
        rows[0, piece : piece + 1, :] = own_row(current_ref[:, span])
        rows[1, piece : piece + 1, :] = own_row(noise_ref[:, span])
    current = rows[0]
    draw = rows[1]
    for copy in range(PER_ROW):
        patch8[copy * PATCH_VALS : (copy + 1) * PATCH_VALS, :] = patch_ref[...]
    spread_lanes = (
        lax.broadcasted_iota(jnp.int32, (LANES, PATCH_VALS), 0) % PATCH_VALS
        == lanes_of((LANES, PATCH_VALS))
    )
    proj8[...] = dot(jnp.where(spread_lanes, 1.0, 0.0).astype(BF16), proj_ref[...]).astype(BF16)

    half = D // 2
    def table_chunk(j, carry):
        place = lax.broadcasted_iota(jnp.int32, (CHUNK_ROWS, D), 0) * PER_ROW + j
        column = lanes_of((CHUNK_ROWS, D))
        first = column < half
        freq = jnp.where(first, column, column - half).astype(F32)
        angle = place.astype(F32) * jnp.exp(-math.log(10000.0) * freq / half)
        table[pl.ds(pl.multiple_of(j * CHUNK_ROWS, CHUNK_ROWS), CHUNK_ROWS), :] = jnp.where(
            first, jnp.sin(angle), jnp.cos(angle)
        )
        return carry

    lax.fori_loop(0, PER_ROW, table_chunk, 0)

    spans = [slice(j * CHUNK_ROWS, (j + 1) * CHUNK_ROWS) for j in range(PER_ROW)]

    def prepare(latent):
        tokens = jnp.concatenate(
            [jnp.where(lane8 == j, latent, 0.0) for j in range(PER_ROW)], axis=0
        ).astype(BF16)
        stream[...] = dot(tokens, patch8[...]) + table[...]
        means, spreads = moments_of(stream, spans)
        for span, mean, scale in zip(spans, means, spreads):
            unit[span] = (stream[span] - mean) * scale

    prepare(current)

    def drain(ref, sem):
        pltpu.make_async_copy(ref, ref, sem).wait()

    relay = jnp.logical_and(holder, jnp.logical_not(direct))

    @pl.when(direct)
    def _():
        drain(tiles_all.at[pl.ds(0, 9 * (CHIPS - 1))], weight_sem.at[1])
        tile_share.start()

    @pl.when(holder)
    def _():
        drain(cond_all.at[:, pl.ds(0, CHIPS - 1)], cond_sem.at[1])

    @pl.when(relay)
    def _():
        tile_share.wait_recv()

    @pl.when(holder)
    def _():
        total = jnp.zeros((2 * CHIPS, LANES), F32)
        for tile in range(FEATURE_TILES):
            lhs = cond_all[tile].reshape(2 * CHIPS, LANES)
            rhs = tiles_all[tile * 64 : (tile + 1) * 64].reshape(LANES, LANES)
            total = total + dot(lhs, rhs)
        mod_send[...] = total.reshape(CHIPS, 2, LANES)
        mods[me] = mod_send[me]

        for chip in peers:
            pltpu.make_async_remote_copy(
                src_ref=mod_send.at[chip],
                dst_ref=mods.at[me],
                send_sem=mod_sem.at[0],
                recv_sem=mod_sem.at[1],
                device_id=at(chip, side),
                device_id_type=MESH,
            ).start()

    @pl.when(holder)
    def _():
        drain(mods.at[pl.ds(0, MOD_TILES - 1)], mod_sem.at[1])

    @pl.when(me >= MOD_TILES)
    def _():
        drain(mods, mod_sem.at[1])

    loads[2].wait()
    loads[3].wait()
    for swap in swaps:
        swap.wait()

    def mod_row(which, moment):
        tiles = [mods[chip] + mods[45] if chip == 13 else mods[chip] for chip in TILE_CHIPS[which]]
        pair = jnp.concatenate(tiles, axis=1)
        return jnp.where(moment == 0, pair[0:1], pair[1:2])

    exponent = HEAD_DIM ** (-0.5) * math.log2(math.e)

    def evaluate(moment):
        shift, scale = mod_row(0, moment), 1.0 + mod_row(1, moment)
        for span in spans:
            normal[span] = (unit[span] * scale + shift).astype(BF16)

        turned[...] = normal[...].T
        weight = [wqkv[part].reshape(D, D) for part in range(3)]
        queries[...] = (dot(weight[0], turned[...]) * exponent).astype(BF16)
        keys[...] = dot(weight[1], turned[...]).astype(BF16).T
        values[...] = dot(weight[2], turned[...]).astype(BF16)

        def score(head):
            low, high = head * HEAD_DIM, (head + 1) * HEAD_DIM
            left = low // LANES * LANES
            right = -(-high // LANES) * LANES
            row = lax.broadcasted_iota(jnp.int32, (right - left, 1), 0) + left
            asked = queries[left:right]
            asked = jnp.where((row >= low) & (row < high), asked, jnp.zeros_like(asked))
            scores[head % 2] = dot(keys[:, left:right], asked)

        def soften(head):
            found = scores[head % 2]
            weights = jnp.exp2(found - jnp.max(found, axis=0, keepdims=True))
            probs[head % 2] = weights.astype(BF16)
            return jnp.sum(weights, axis=0, keepdims=True)

        def apply(head, whole):
            low, high = head * HEAD_DIM, (head + 1) * HEAD_DIM
            first = low // 16 * 16
            result = dot(values[first : first + 80], probs[head % 2])
            mixed[low:high] = result[low - first : high - first] * (1.0 / whole)

        score(0)
        before = None
        for head in range(HEADS):
            if head + 1 < HEADS:
                score(head + 1)
            whole = soften(head)
            if head:
                apply(head - 1, before)
            before = whole
        apply(HEADS - 1, before)

        attended = lax.dot_general(
            mixed[...].astype(BF16),
            wout[...].reshape(D, D),
            (((0,), (0,)), ((), ())),
            preferred_element_type=F32,
        )
        stream[...] = stream[...] + mod_row(2, moment) * attended
        shift, scale = mod_row(3, moment), 1.0 + mod_row(4, moment)
        means, spreads = moments_of(stream, spans)
        for span, mean, spread_inv in zip(spans, means, spreads):
            normal[span] = ((stream[span] - mean) * spread_inv * scale + shift).astype(BF16)
        guessed = dot_t(normal[...], proj8[...])
        result = jnp.zeros((CHUNK_ROWS, LANES), F32)
        for j in range(PER_ROW):
            result = result + jnp.where(
                lane8 == j, guessed[j * CHUNK_ROWS : (j + 1) * CHUNK_ROWS], 0.0
            )
        return result

    spread = jnp.sqrt(step_size * beta_at(time_now)) * draw


    def one_moment(moment, carry):
        guess = evaluate(moment)
        rows[4] = guess

        @pl.when(moment == 0)
        def _():
            rows[3] = guess
            beta = beta_at(time_now)
            drift_now = 0.5 * beta * rows[0] - beta * guess / sigma_at(time_now)
            euler_now = rows[0] + step_size * drift_now + spread
            rows[2] = euler_now
            prepare(euler_now)

        return carry

    lax.fori_loop(0, 2, one_moment, 0)

    current = rows[0]
    beta = beta_at(time_now)
    drift_now = 0.5 * beta * current - beta * rows[3] / sigma_at(time_now)
    euler = rows[2]
    beta_then = beta_at(later)
    drift_later = 0.5 * beta_then * euler - beta_then * rows[4] / sigma_at(later)
    heun = current + 0.5 * step_size * (drift_now + drift_later) + spread
    scale_ref = jnp.maximum(tol_abs, tol_rel * jnp.maximum(jnp.abs(heun), jnp.abs(current)))
    gap = (euler - heun) / scale_ref
    squares = jnp.sum(jnp.sum(gap * gap, axis=1, keepdims=True), axis=0, keepdims=True)
    error = jnp.sqrt(squares / LATENT)
    taken = jnp.full((CHUNK_ROWS, LANES), accept_ref[side], jnp.int32) == 1
    finals[side, :CHUNK_ROWS] = jnp.where(taken, heun, current)
    finals[side, CHUNK_ROWS:] = jnp.broadcast_to(error, (8, LANES))
    final_swap = pltpu.make_async_remote_copy(
        src_ref=finals.at[side],
        dst_ref=finals.at[side],
        send_sem=final_sem.at[0],
        recv_sem=final_sem.at[1],
        device_id=at(me, other),
        device_id_type=MESH,
    )
    final_swap.start()

    @pl.when(me >= MOD_TILES)
    def _():
        drain(cond_all.at[:, pl.ds(0, MOD_TILES)], cond_sem.at[0])

    @pl.when(me < MOD_TILES)
    def _():
        drain(cond_all.at[:, pl.ds(0, MOD_TILES - 1)], cond_sem.at[0])
        drain(mod_send.at[pl.ds(0, CHIPS - 1)], mod_sem.at[0])

    @pl.when(direct)
    def _():
        drain(tiles_all.at[pl.ds(0, 9 * (SIDE_TILES - 1))], weight_sem.at[0])
        tile_share.wait_send()

    @pl.when(jnp.logical_not(direct))
    def _():
        drain(tiles_all.at[pl.ds(0, 9 * SIDE_TILES)], weight_sem.at[0])

    final_swap.wait()
    for latent in range(2):
        for piece in range(CHUNK_ROWS):
            state_ref[latent : latent + 1, piece * LANES : (piece + 1) * LANES] = finals[
                latent, piece : piece + 1, :
            ]
        error_ref[latent : latent + 1, :] = finals[latent, CHUNK_ROWS : CHUNK_ROWS + 1, :]


def shards(
    current,
    noise_draw,
    labels,
    time_now,
    step_size,
    accept,
    patch_weight,
    time_in,
    time_out,
    qkv_weight,
    out_weight,
    ada_weight,
    final_ada,
    final_proj,
):
    vmem = pl.BlockSpec(memory_space=pltpu.VMEM)
    place = pl.BlockSpec(memory_space=pl.ANY)
    state, error = pl.pallas_call(
        kernel,
        out_shape=(
            pltpu.VMEM((2, LATENT), F32),
            pltpu.VMEM((2, LANES), F32),
        ),
        in_specs=[place] * 14,
        out_specs=(vmem, vmem),
        scratch_shapes=[
            pltpu.SMEM((2,), F32),
            pltpu.SMEM((2,), F32),
            pltpu.SMEM((2,), jnp.int32),
            pltpu.VMEM((2, LATENT), F32),
            pltpu.VMEM((2, LATENT), F32),
            pltpu.VMEM((2, D), BF16),
            pltpu.VMEM((PATCH_VALS, D), BF16),
            pltpu.VMEM((PATCH_VALS, D), BF16),
            pltpu.VMEM((1, 18, 3 * HALF), BF16),
            pltpu.VMEM((18, D), BF16),
            pltpu.VMEM((FREQ, D), BF16),
            pltpu.VMEM((D, D), BF16),
            pltpu.VMEM((3, GROUPS, HALF, D), BF16),
            pltpu.VMEM((GROUPS, HALF, D), BF16),
            pltpu.VMEM((MOD_TILES, 9, 2, LANES), BF16),
            pltpu.VMEM((FEATURE_TILES, 2, LANES), BF16),
            pltpu.VMEM((FEATURE_TILES, CHIPS, 2, LANES), BF16),
            pltpu.VMEM((9 * CHIPS, 2, LANES), BF16),
            pltpu.VMEM((CHIPS, 2, LANES), F32),
            pltpu.VMEM((MOD_TILES, 2, LANES), F32),
            pltpu.VMEM((2, CHUNK_ROWS + 8, LANES), F32),
            pltpu.VMEM((LANES, D), BF16),
            pltpu.VMEM((LANES, D), BF16),
            pltpu.VMEM((TOK, D), F32),
            pltpu.VMEM((TOK, D), F32),
            pltpu.VMEM((TOK, D), F32),
            pltpu.VMEM((TOK, D), BF16),
            pltpu.VMEM((D, TOK), BF16),
            pltpu.VMEM((TOK, D), BF16),
            pltpu.VMEM((D, TOK), BF16),
            pltpu.VMEM((D, TOK), F32),
            pltpu.VMEM((D, TOK), BF16),
            pltpu.VMEM((2, TOK, TOK), F32),
            pltpu.VMEM((2, TOK, TOK), BF16),
            pltpu.VMEM((5, CHUNK_ROWS, LANES), F32),
            pltpu.SemaphoreType.DMA((4,)),
            pltpu.SemaphoreType.DMA((10,)),
            pltpu.SemaphoreType.DMA((2,)),
            pltpu.SemaphoreType.DMA((4,)),
            pltpu.SemaphoreType.DMA((2,)),
            pltpu.SemaphoreType.DMA((2,)),
            pltpu.SemaphoreType.DMA((2,)),
            pltpu.SemaphoreType.DMA((2,)),
        ],
        compiler_params=pltpu.CompilerParams(
            collective_id=0, has_side_effects=True, vmem_limit_bytes=60 * 1024 * 1024
        ),
        name="heun_step",
    )(
        time_now,
        step_size,
        accept,
        current,
        noise_draw,
        labels,
        patch_weight,
        final_proj.T,
        ada_weight,
        final_ada,
        time_in,
        time_out,
        qkv_weight[0].transpose(1, 2, 0),
        out_weight[0].T,
    )
    return state, error[:, 0]


def solution(mesh):
    in_specs = (
        P("dp", None),
        P("dp", None),
        P("dp", None),
        P("dp"),
        P("dp"),
        P("dp"),
        P(),
        P(),
        P(),
        P(None, None, None, "tensor"),
        P(None, None, "tensor"),
        P(None, "dp", "tensor"),
        P("dp", "tensor"),
        P(),
    )
    out_specs = (P("dp", None), P("dp"))
    return jax.shard_map(shards, mesh=mesh, in_specs=in_specs, out_specs=out_specs, check_vma=False)
```

```python
import functools
import math

import jax
import jax.numpy as jnp
from jax import lax
from jax.experimental import pallas as pl
from jax.experimental.pallas import tpu as pltpu
from jax.sharding import PartitionSpec as P

MESH = pl.DeviceIdType.MESH
F32 = jnp.float32
BF16 = jnp.bfloat16

D = 1152
TOK = 256
PATCH_VALS = 16
FREQ = 256
HEADS = 16
HEAD_DIM = 72
LATENT = 4096
GROUPS = 2
HALF = D // GROUPS
FOUR = 4 * HEAD_DIM
LANES = 128
CHUNK_ROWS = LATENT // LANES
PER_ROW = LANES // PATCH_VALS
FEATURE_TILES = D // LANES
MOD_TILES = 46
SIDE_TILES = 23
CHIPS = 64
TILE_CHIPS = (
    tuple(range(9)),
    (9, 10, 11, 12, 13, 23, 24, 25, 26),
    tuple(range(27, 36)),
    tuple(range(14, 23)),
    tuple(range(36, 45)),
)

beta_low = 0.1
beta_high = 20.0
tol_abs = 0.0078
tol_rel = 0.05
norm_eps = 1e-06


def beta_at(moments):
    return beta_low + (beta_high - beta_low) * moments


def sigma_at(moments):
    integral = beta_low * moments + 0.5 * (beta_high - beta_low) * moments * moments
    return jnp.sqrt(1.0 - jnp.exp(-integral))


def lanes_of(shape):
    return lax.broadcasted_iota(jnp.int32, shape, len(shape) - 1)


def silu(values):
    return values / (1.0 + jnp.exp(-values))


def moments_of(ref, spans):
    means = [jnp.sum(ref[span], axis=-1, keepdims=True) * (1.0 / D) for span in spans]
    spreads = []
    for span, mean in zip(spans, means):
        centred = ref[span] - mean
        spread_sq = jnp.sum(centred * centred, axis=-1, keepdims=True) * (1.0 / D)
        spreads.append(lax.rsqrt(spread_sq + norm_eps))
    return means, spreads


def dot(a, b):
    return jnp.dot(a, b, preferred_element_type=F32)


def dot_t(a, b):
    return lax.dot_general(a, b, (((1,), (1,)), ((), ())), preferred_element_type=F32)


OFFSETS = sorted(
    ((z, y, x) for z in (2, 1, 3, 0) for y in (2, 1, 3, 0) for x in (2, 1, 3, 0) if z + y + x),
    key=lambda offset: -sum(min(step, 4 - step) for step in offset),
)


def kernel(
    now_in,
    step_in,
    accept_in,
    current_in,
    noise_in,
    labels_in,
    patch_in,
    proj_in,
    ada_in,
    final_in,
    time_in_ref,
    time_out_ref,
    qkv_ref,
    out_ref,
    state_ref,
    error_ref,
    now_ref,
    step_ref,
    accept_ref,
    current_ref,
    noise_ref,
    labels_ref,
    patch_ref,
    proj_ref,
    ada_ref,
    final_ref,
    time_in,
    time_out,
    wqkv,
    wout,
    stage,
    cond_send,
    cond_all,
    tiles_all,
    mod_send,
    mods,
    finals,
    patch8,
    proj8,
    table,
    unit,
    stream,
    normal,
    queries,
    keys,
    values,
    mixed,
    turned,
    scores,
    probs,
    rows,
    local_sem,
    small_sem,
    tile_sem,
    swap_sem,
    cond_sem,
    weight_sem,
    mod_sem,
    final_sem,
):
    me = lax.axis_index("dp")
    side = lax.axis_index("tensor")
    other = 1 - side

    def at(chip, core):
        return {"dp": chip, "tensor": core}

    def own_row(pair):
        return jnp.where(side == 0, pair[0:1], pair[1:2])

    own_half = pl.ds(pl.multiple_of(side * HALF, HALF), HALF)
    loads = [
        pltpu.make_async_copy(time_in_ref, time_in, local_sem.at[0]),
        pltpu.make_async_copy(time_out_ref, time_out, local_sem.at[1]),
        pltpu.make_async_copy(qkv_ref, wqkv.at[:, side], local_sem.at[2]),
        pltpu.make_async_copy(out_ref, wout.at[own_half], local_sem.at[3]),
    ]
    for copy in loads[:2]:
        copy.start()
    small = [
        pltpu.make_async_copy(source, target, small_sem.at[slot])
        for slot, (source, target) in enumerate(
            (
                (now_in, now_ref),
                (step_in, step_ref),
                (ada_in, ada_ref),
                (final_in, final_ref),
                (labels_in, labels_ref),
                (current_in, current_ref),
                (noise_in, noise_ref),
                (patch_in, patch_ref),
                (proj_in, proj_ref),
                (accept_in, accept_ref),
            )
        )
    ]
    for copy in small:
        copy.start()

    barrier = pltpu.get_barrier_semaphore()
    pl.semaphore_signal(barrier, inc=1, device_id=at(me, other), device_id_type=MESH)

    along_x = [lax.rem(me + step, 4) for step in range(4)]
    along_y = [lax.rem(me // 4 + step, 4) * 4 for step in range(4)]
    along_z = [lax.rem(me // 16 + step, 4) * 16 for step in range(4)]
    peers = [along_z[z] + along_y[y] + along_x[x] for z, y, x in OFFSETS]
    holder = me < MOD_TILES

    @pl.when(holder)
    def _():
        for chip in peers:
            pl.semaphore_signal(barrier, inc=1, device_id=at(chip, side), device_id_type=MESH)

    small[2].wait()
    small[3].wait()

    def put(tile, values):
        for pair in range(9):
            stage[tile, pair] = values[2 * pair : 2 * pair + 2]

    blank = jnp.zeros((18, 64), BF16)

    @pl.when(side == 0)
    def _():
        for tile in range(13):
            put(tile, ada_ref[0, :, tile * LANES : (tile + 1) * LANES])
        for tile in range(FEATURE_TILES):
            put(14 + tile, final_ref[:, tile * LANES : (tile + 1) * LANES])
        put(13, jnp.concatenate([ada_ref[0, :, 13 * LANES : 13 * LANES + 64], blank], axis=1))

    @pl.when(side == 1)
    def _():
        put(MOD_TILES - 1, jnp.concatenate([blank, ada_ref[0, :, 0:64]], axis=1))
        for tile in range(1, 14):
            start = tile * LANES - 64
            put(22 + tile, ada_ref[0, :, start : start + LANES])
        for tile in range(FEATURE_TILES):
            put(36 + tile, final_ref[:, tile * LANES : (tile + 1) * LANES])

    for slot in (0, 1, 4):
        small[slot].wait()
    time_now = jnp.full((1, LANES), now_ref[side], F32)
    step_size = jnp.full((1, LANES), step_ref[side], F32)
    later = time_now - step_size
    moments = jnp.concatenate([time_now, later, jnp.zeros((6, LANES), F32)], axis=0)

    def condition():
        index = lanes_of((8, LANES)).astype(F32)
        rates = jnp.exp(-math.log(10000.0) * index / (FREQ // 2))
        angles = 1000.0 * moments * rates
        features = jnp.concatenate([jnp.cos(angles), jnp.sin(angles)], axis=1).astype(BF16)
        loads[0].wait()
        hidden = silu(dot(features, time_in[...])).astype(BF16)
        loads[1].wait()
        loads[2].start()
        loads[3].start()
        label = own_row(labels_ref[...].astype(F32))
        cond = silu(label + dot(hidden, time_out[...])).astype(BF16)
        for tile in range(FEATURE_TILES):
            piece = cond[0:2, tile * LANES : (tile + 1) * LANES]
            cond_send[tile] = piece
            cond_all[me, tile] = piece

    early = me < CHIPS // 2
    pl.when(early)(condition)

    @pl.when(holder)
    def _():
        pl.semaphore_wait(barrier, MOD_TILES)

    @pl.when(jnp.logical_not(holder))
    def _():
        pl.semaphore_wait(barrier, MOD_TILES + 1)

    base = side * SIDE_TILES
    direct = jnp.logical_and(me >= base, me < base + SIDE_TILES)

    def send_tile(step):
        chip = base + lax.rem(me + step, SIDE_TILES)
        pltpu.make_async_remote_copy(
            src_ref=stage.at[chip],
            dst_ref=tiles_all.at[pl.ds(me * 9, 9)],
            send_sem=weight_sem.at[0],
            recv_sem=weight_sem.at[1],
            device_id=at(chip, side),
            device_id_type=MESH,
        ).start()

    def send_rows(step):
        pltpu.make_async_remote_copy(
            src_ref=cond_send,
            dst_ref=cond_all.at[me],
            send_sem=cond_sem.at[0],
            recv_sem=cond_sem.at[1],
            device_id=at(lax.rem(me + step, MOD_TILES), side),
            device_id_type=MESH,
        ).start()

    for step in range(1, SIDE_TILES):
        send_tile(step)

    @pl.when(jnp.logical_not(direct))
    def _():
        send_tile(0)

    @pl.when(direct)
    def _():
        tiles_all[pl.ds(me * 9, 9)] = stage[me]

    pl.when(jnp.logical_not(early))(condition)

    for step in range(1, MOD_TILES):
        send_rows(step)

    @pl.when(jnp.logical_not(holder))
    def _():
        send_rows(0)

    tile_share = pltpu.make_async_remote_copy(
        src_ref=tiles_all,
        dst_ref=tiles_all,
        send_sem=tile_sem.at[0],
        recv_sem=tile_sem.at[1],
        device_id=at(me, other),
        device_id_type=MESH,
    )

    swaps = []
    for slot, (src, dst) in enumerate(((qkv_ref, wqkv.at[:, side]), (out_ref, wout.at[own_half]))):
        swaps.append(
            pltpu.make_async_remote_copy(
                src_ref=src,
                dst_ref=dst,
                send_sem=swap_sem.at[slot],
                recv_sem=swap_sem.at[2 + slot],
                device_id=at(me, other),
                device_id_type=MESH,
            )
        )
        swaps[-1].start()

    for copy in small[5:]:
        copy.wait()
    lane8 = lanes_of((CHUNK_ROWS, LANES)) // PATCH_VALS
    for piece in range(CHUNK_ROWS):
        span = slice(piece * LANES, (piece + 1) * LANES)
        rows[0, piece : piece + 1, :] = own_row(current_ref[:, span])
        rows[1, piece : piece + 1, :] = own_row(noise_ref[:, span])
    current = rows[0]
    draw = rows[1]
    for copy in range(PER_ROW):
        patch8[copy * PATCH_VALS : (copy + 1) * PATCH_VALS, :] = patch_ref[...]
    spread_lanes = (
        lax.broadcasted_iota(jnp.int32, (LANES, PATCH_VALS), 0) % PATCH_VALS
        == lanes_of((LANES, PATCH_VALS))
    )
    proj8[...] = dot(jnp.where(spread_lanes, 1.0, 0.0).astype(BF16), proj_ref[...]).astype(BF16)

    half = D // 2
    queries[...] = jnp.zeros_like(queries)

    def table_chunk(j, carry):
        place = lax.broadcasted_iota(jnp.int32, (CHUNK_ROWS, D), 0) * PER_ROW + j
        column = lanes_of((CHUNK_ROWS, D))
        first = column < half
        freq = jnp.where(first, column, column - half).astype(F32)
        angle = place.astype(F32) * jnp.exp(-math.log(10000.0) * freq / half)
        table[pl.ds(pl.multiple_of(j * CHUNK_ROWS, CHUNK_ROWS), CHUNK_ROWS), :] = jnp.where(
            first, jnp.sin(angle), jnp.cos(angle)
        )
        return carry

    lax.fori_loop(0, PER_ROW, table_chunk, 0)

    spans = [slice(j * CHUNK_ROWS, (j + 1) * CHUNK_ROWS) for j in range(PER_ROW)]

    def prepare(latent):
        tokens = jnp.concatenate(
            [jnp.where(lane8 == j, latent, 0.0) for j in range(PER_ROW)], axis=0
        ).astype(BF16)
        stream[...] = dot(tokens, patch8[...]) + table[...]
        means, spreads = moments_of(stream, spans)
        for span, mean, scale in zip(spans, means, spreads):
            unit[span] = (stream[span] - mean) * scale

    prepare(current)

    def drain(ref, sem):
        pltpu.make_async_copy(ref, ref, sem).wait()

    relay = jnp.logical_and(holder, jnp.logical_not(direct))

    @pl.when(direct)
    def _():
        drain(tiles_all.at[pl.ds(0, 9 * (CHIPS - 1))], weight_sem.at[1])
        tile_share.start()

    @pl.when(holder)
    def _():
        drain(cond_all.at[pl.ds(0, CHIPS - 1)], cond_sem.at[1])

    @pl.when(relay)
    def _():
        tile_share.wait_recv()

    @pl.when(holder)
    def _():
        total = jnp.zeros((2 * CHIPS, LANES), F32)
        for tile in range(FEATURE_TILES):
            lhs = cond_all[:, tile].reshape(2 * CHIPS, LANES)
            rhs = tiles_all[tile * 64 : (tile + 1) * 64].reshape(LANES, LANES)
            total = total + dot(lhs, rhs)
        mod_send[...] = total.reshape(CHIPS, 2, LANES)
        mods[me] = mod_send[me]

        for chip in peers:
            pltpu.make_async_remote_copy(
                src_ref=mod_send.at[chip],
                dst_ref=mods.at[me],
                send_sem=mod_sem.at[0],
                recv_sem=mod_sem.at[1],
                device_id=at(chip, side),
                device_id_type=MESH,
            ).start()

    @pl.when(holder)
    def _():
        drain(mods.at[pl.ds(0, MOD_TILES - 1)], mod_sem.at[1])

    @pl.when(me >= MOD_TILES)
    def _():
        drain(mods, mod_sem.at[1])

    loads[2].wait()
    loads[3].wait()
    for swap in swaps:
        swap.wait()

    def mod_row(which, moment):
        tiles = [mods[chip] + mods[45] if chip == 13 else mods[chip] for chip in TILE_CHIPS[which]]
        pair = jnp.concatenate(tiles, axis=1)
        return jnp.where(moment == 0, pair[0:1], pair[1:2])

    nothing = jnp.zeros((8, TOK), F32)
    exponent = HEAD_DIM ** (-0.5) * math.log2(math.e)

    def evaluate(moment):
        shift, scale = mod_row(0, moment), 1.0 + mod_row(1, moment)
        for span in spans:
            normal[span] = (unit[span] * scale + shift).astype(BF16)

        turned[...] = normal[...].T
        keys[...] = dot(wqkv[1].reshape(D, D), turned[...]).astype(BF16).T

        def project(four):
            group, row = four // 2, four % 2 * FOUR
            asked = dot(wqkv[0, group, row : row + FOUR], turned[...]) * exponent
            given = dot(wqkv[2, group, row : row + FOUR], turned[...])
            for place in range(4):
                head = 4 * four + place
                low = head * HEAD_DIM
                span = slice(place * HEAD_DIM, (place + 1) * HEAD_DIM)
                rows72 = [asked[span], nothing] if low % 16 == 0 else [nothing, asked[span]]
                start = low // 16 * 16 - low // LANES * LANES
                queries[head, start : start + 80] = jnp.concatenate(rows72, axis=0).astype(BF16)
                values[head] = jnp.concatenate([given[span], nothing + 1.0], axis=0).astype(BF16)

        def leave():
            return lax.dot_general(
                mixed[...].astype(BF16),
                wout[...],
                (((0,), (0,)), ((), ())),
                preferred_element_type=F32,
            )

        def score(head):
            low, high = head * HEAD_DIM, (head + 1) * HEAD_DIM
            left = low // LANES * LANES
            right = -(-high // LANES) * LANES
            scores[head % 2] = dot(keys[:, left:right], queries[head, : right - left])

        def soften(head):
            found = scores[head % 2]
            weights = jnp.exp2(found - jnp.max(found, axis=0, keepdims=True))
            probs[head % 2] = weights.astype(BF16)

        def apply(head):
            result = dot(values[head], probs[head % 2])
            mixed[head * HEAD_DIM : (head + 1) * HEAD_DIM] = result[:HEAD_DIM] * (
                1.0 / result[HEAD_DIM : HEAD_DIM + 1]
            )

        project(0)
        score(0)
        for head in range(HEADS):
            if head % 4 == 0 and head + 4 < HEADS:
                project(head // 4 + 1)
            if head + 1 < HEADS:
                score(head + 1)
            soften(head)
            if head:
                apply(head - 1)
        apply(HEADS - 1)
        stream[...] = stream[...] + mod_row(2, moment) * leave()
        shift, scale = mod_row(3, moment), 1.0 + mod_row(4, moment)
        means, spreads = moments_of(stream, spans)
        for span, mean, spread_inv in zip(spans, means, spreads):
            normal[span] = ((stream[span] - mean) * spread_inv * scale + shift).astype(BF16)
        guessed = dot_t(normal[...], proj8[...])
        result = jnp.zeros((CHUNK_ROWS, LANES), F32)
        for j in range(PER_ROW):
            result = result + jnp.where(
                lane8 == j, guessed[j * CHUNK_ROWS : (j + 1) * CHUNK_ROWS], 0.0
            )
        return result

    spread = jnp.sqrt(step_size * beta_at(time_now)) * draw


    def one_moment(moment, carry):
        guess = evaluate(moment)
        rows[4] = guess

        @pl.when(moment == 0)
        def _():
            rows[3] = guess
            beta = beta_at(time_now)
            drift_now = 0.5 * beta * rows[0] - beta * guess / sigma_at(time_now)
            euler_now = rows[0] + step_size * drift_now + spread
            rows[2] = euler_now
            prepare(euler_now)

        return carry

    lax.fori_loop(0, 2, one_moment, 0)

    current = rows[0]
    beta = beta_at(time_now)
    drift_now = 0.5 * beta * current - beta * rows[3] / sigma_at(time_now)
    euler = rows[2]
    beta_then = beta_at(later)
    drift_later = 0.5 * beta_then * euler - beta_then * rows[4] / sigma_at(later)
    heun = current + 0.5 * step_size * (drift_now + drift_later) + spread
    scale_ref = jnp.maximum(tol_abs, tol_rel * jnp.maximum(jnp.abs(heun), jnp.abs(current)))
    gap = (euler - heun) / scale_ref
    squares = jnp.sum(jnp.sum(gap * gap, axis=1, keepdims=True), axis=0, keepdims=True)
    error = jnp.sqrt(squares / LATENT)
    taken = jnp.full((CHUNK_ROWS, LANES), accept_ref[side], jnp.int32) == 1
    finals[side, :CHUNK_ROWS] = jnp.where(taken, heun, current)
    finals[side, CHUNK_ROWS:] = jnp.broadcast_to(error, (8, LANES))
    final_swap = pltpu.make_async_remote_copy(
        src_ref=finals.at[side],
        dst_ref=finals.at[side],
        send_sem=final_sem.at[0],
        recv_sem=final_sem.at[1],
        device_id=at(me, other),
        device_id_type=MESH,
    )
    final_swap.start()

    @pl.when(me >= MOD_TILES)
    def _():
        drain(cond_all.at[pl.ds(0, MOD_TILES)], cond_sem.at[0])

    @pl.when(me < MOD_TILES)
    def _():
        drain(cond_all.at[pl.ds(0, MOD_TILES - 1)], cond_sem.at[0])
        drain(mod_send.at[pl.ds(0, CHIPS - 1)], mod_sem.at[0])

    @pl.when(direct)
    def _():
        drain(tiles_all.at[pl.ds(0, 9 * (SIDE_TILES - 1))], weight_sem.at[0])
        tile_share.wait_send()

    @pl.when(jnp.logical_not(direct))
    def _():
        drain(tiles_all.at[pl.ds(0, 9 * SIDE_TILES)], weight_sem.at[0])

    final_swap.wait()
    for latent in range(2):
        for piece in range(CHUNK_ROWS):
            state_ref[latent : latent + 1, piece * LANES : (piece + 1) * LANES] = finals[
                latent, piece : piece + 1, :
            ]
        error_ref[latent : latent + 1, :] = finals[latent, CHUNK_ROWS : CHUNK_ROWS + 1, :]


def shards(
    current,
    noise_draw,
    labels,
    time_now,
    step_size,
    accept,
    patch_weight,
    time_in,
    time_out,
    qkv_weight,
    out_weight,
    ada_weight,
    final_ada,
    final_proj,
):
    vmem = pl.BlockSpec(memory_space=pltpu.VMEM)
    place = pl.BlockSpec(memory_space=pl.ANY)
    state, error = pl.pallas_call(
        kernel,
        out_shape=(
            pltpu.VMEM((2, LATENT), F32),
            pltpu.VMEM((2, LANES), F32),
        ),
        in_specs=[place] * 14,
        out_specs=(vmem, vmem),
        scratch_shapes=[
            pltpu.SMEM((2,), F32),
            pltpu.SMEM((2,), F32),
            pltpu.SMEM((2,), jnp.int32),
            pltpu.VMEM((2, LATENT), F32),
            pltpu.VMEM((2, LATENT), F32),
            pltpu.VMEM((2, D), BF16),
            pltpu.VMEM((PATCH_VALS, D), BF16),
            pltpu.VMEM((PATCH_VALS, D), BF16),
            pltpu.VMEM((1, 18, 3 * HALF), BF16),
            pltpu.VMEM((18, D), BF16),
            pltpu.VMEM((FREQ, D), BF16),
            pltpu.VMEM((D, D), BF16),
            pltpu.VMEM((3, GROUPS, HALF, D), BF16),
            pltpu.VMEM((D, D), BF16),
            pltpu.VMEM((MOD_TILES, 9, 2, LANES), BF16),
            pltpu.VMEM((FEATURE_TILES, 2, LANES), BF16),
            pltpu.VMEM((CHIPS, FEATURE_TILES, 2, LANES), BF16),
            pltpu.VMEM((9 * CHIPS, 2, LANES), BF16),
            pltpu.VMEM((CHIPS, 2, LANES), F32),
            pltpu.VMEM((MOD_TILES, 2, LANES), F32),
            pltpu.VMEM((2, CHUNK_ROWS + 8, LANES), F32),
            pltpu.VMEM((LANES, D), BF16),
            pltpu.VMEM((LANES, D), BF16),
            pltpu.VMEM((TOK, D), F32),
            pltpu.VMEM((TOK, D), F32),
            pltpu.VMEM((TOK, D), F32),
            pltpu.VMEM((TOK, D), BF16),
            pltpu.VMEM((HEADS, 2 * LANES, TOK), BF16),
            pltpu.VMEM((TOK, D), BF16),
            pltpu.VMEM((HEADS, 80, TOK), BF16),
            pltpu.VMEM((D, TOK), F32),
            pltpu.VMEM((D, TOK), BF16),
            pltpu.VMEM((2, TOK, TOK), F32),
            pltpu.VMEM((2, TOK, TOK), BF16),
            pltpu.VMEM((5, CHUNK_ROWS, LANES), F32),
            pltpu.SemaphoreType.DMA((4,)),
            pltpu.SemaphoreType.DMA((10,)),
            pltpu.SemaphoreType.DMA((2,)),
            pltpu.SemaphoreType.DMA((4,)),
            pltpu.SemaphoreType.DMA((2,)),
            pltpu.SemaphoreType.DMA((2,)),
            pltpu.SemaphoreType.DMA((2,)),
            pltpu.SemaphoreType.DMA((2,)),
        ],
        compiler_params=pltpu.CompilerParams(
            collective_id=0, has_side_effects=True, vmem_limit_bytes=60 * 1024 * 1024
        ),
        name="heun_step",
    )(
        time_now,
        step_size,
        accept,
        current,
        noise_draw,
        labels,
        patch_weight,
        final_proj.T,
        ada_weight,
        final_ada,
        time_in,
        time_out,
        qkv_weight[0].transpose(1, 2, 0),
        out_weight[0].T,
    )
    return state, error[:, 0]


def solution(mesh):
    in_specs = (
        P("dp", None),
        P("dp", None),
        P("dp", None),
        P("dp"),
        P("dp"),
        P("dp"),
        P(),
        P(),
        P(),
        P(None, None, None, "tensor"),
        P(None, None, "tensor"),
        P(None, "dp", "tensor"),
        P("dp", "tensor"),
        P(),
    )
    out_specs = (P("dp", None), P("dp"))
    return jax.shard_map(shards, mesh=mesh, in_specs=in_specs, out_specs=out_specs, check_vma=False)
```

```python
import functools
import math

import jax
import jax.numpy as jnp
from jax import lax
from jax.experimental import pallas as pl
from jax.experimental.pallas import tpu as pltpu
from jax.sharding import PartitionSpec as P

MESH = pl.DeviceIdType.MESH
F32 = jnp.float32
BF16 = jnp.bfloat16

D = 1152
TOK = 256
PATCH_VALS = 16
FREQ = 256
HEADS = 16
HEAD_DIM = 72
LATENT = 4096
GROUPS = 2
HALF = D // GROUPS
FOUR = 4 * HEAD_DIM
LANES = 128
CHUNK_ROWS = LATENT // LANES
PER_ROW = LANES // PATCH_VALS
FEATURE_TILES = D // LANES
MOD_TILES = 46
SIDE_TILES = 23
CHIPS = 64
TILE_CHIPS = (
    tuple(range(9)),
    (9, 10, 11, 12, 13, 23, 24, 25, 26),
    tuple(range(27, 36)),
    tuple(range(14, 23)),
    tuple(range(36, 45)),
)

beta_low = 0.1
beta_high = 20.0
tol_abs = 0.0078
tol_rel = 0.05
norm_eps = 1e-06


def beta_at(moments):
    return beta_low + (beta_high - beta_low) * moments


def sigma_at(moments):
    integral = beta_low * moments + 0.5 * (beta_high - beta_low) * moments * moments
    return jnp.sqrt(1.0 - jnp.exp(-integral))


def lanes_of(shape):
    return lax.broadcasted_iota(jnp.int32, shape, len(shape) - 1)


def silu(values):
    return values / (1.0 + jnp.exp(-values))


def moments_of(ref, spans):
    means = [jnp.sum(ref[span], axis=-1, keepdims=True) * (1.0 / D) for span in spans]
    spreads = []
    for span, mean in zip(spans, means):
        centred = ref[span] - mean
        spread_sq = jnp.sum(centred * centred, axis=-1, keepdims=True) * (1.0 / D)
        spreads.append(lax.rsqrt(spread_sq + norm_eps))
    return means, spreads


def dot(a, b):
    return jnp.dot(a, b, preferred_element_type=F32)


def dot_t(a, b):
    return lax.dot_general(a, b, (((1,), (1,)), ((), ())), preferred_element_type=F32)


OFFSETS = sorted(
    ((z, y, x) for z in (2, 1, 3, 0) for y in (2, 1, 3, 0) for x in (2, 1, 3, 0) if z + y + x),
    key=lambda offset: -sum(min(step, 4 - step) for step in offset),
)


def kernel(
    now_in,
    step_in,
    accept_in,
    current_in,
    noise_in,
    labels_in,
    patch_in,
    proj_in,
    ada_in,
    final_in,
    time_in_ref,
    time_out_ref,
    qkv_ref,
    out_ref,
    state_ref,
    error_ref,
    now_ref,
    step_ref,
    accept_ref,
    current_ref,
    noise_ref,
    labels_ref,
    patch_ref,
    proj_ref,
    ada_ref,
    final_ref,
    time_in,
    time_out,
    wqkv,
    wout,
    stage,
    cond_send,
    cond_all,
    tiles_all,
    mod_send,
    mods,
    finals,
    patch8,
    proj8,
    table,
    unit,
    stream,
    normal,
    queries,
    keys,
    values,
    mixed,
    turned,
    scores,
    probs,
    rows,
    local_sem,
    small_sem,
    tile_sem,
    swap_sem,
    cond_sem,
    weight_sem,
    mod_sem,
    final_sem,
):
    me = lax.axis_index("dp")
    side = lax.axis_index("tensor")
    other = 1 - side

    def at(chip, core):
        return {"dp": chip, "tensor": core}

    def own_row(pair):
        return jnp.where(side == 0, pair[0:1], pair[1:2])

    own_half = pl.ds(pl.multiple_of(side * HALF, HALF), HALF)
    loads = [
        pltpu.make_async_copy(time_in_ref, time_in, local_sem.at[0]),
        pltpu.make_async_copy(time_out_ref, time_out, local_sem.at[1]),
        pltpu.make_async_copy(qkv_ref, wqkv.at[:, side], local_sem.at[2]),
        pltpu.make_async_copy(out_ref, wout.at[own_half], local_sem.at[3]),
    ]
    for copy in loads[:2]:
        copy.start()
    small = [
        pltpu.make_async_copy(source, target, small_sem.at[slot])
        for slot, (source, target) in enumerate(
            (
                (now_in, now_ref),
                (step_in, step_ref),
                (ada_in, ada_ref),
                (final_in, final_ref),
                (labels_in, labels_ref),
                (current_in, current_ref),
                (noise_in, noise_ref),
                (patch_in, patch_ref),
                (proj_in, proj_ref),
                (accept_in, accept_ref),
            )
        )
    ]
    for copy in small:
        copy.start()

    barrier = pltpu.get_barrier_semaphore()
    pl.semaphore_signal(barrier, inc=1, device_id=at(me, other), device_id_type=MESH)

    along_x = [lax.rem(me + step, 4) for step in range(4)]
    along_y = [lax.rem(me // 4 + step, 4) * 4 for step in range(4)]
    along_z = [lax.rem(me // 16 + step, 4) * 16 for step in range(4)]
    peers = [along_z[z] + along_y[y] + along_x[x] for z, y, x in OFFSETS]
    holder = me < MOD_TILES

    @pl.when(holder)
    def _():
        for chip in peers:
            pl.semaphore_signal(barrier, inc=1, device_id=at(chip, side), device_id_type=MESH)

    small[2].wait()
    small[3].wait()

    def put(tile, values):
        for pair in range(9):
            stage[tile, pair] = values[2 * pair : 2 * pair + 2]

    blank = jnp.zeros((18, 64), BF16)

    @pl.when(side == 0)
    def _():
        for tile in range(13):
            put(tile, ada_ref[0, :, tile * LANES : (tile + 1) * LANES])
        for tile in range(FEATURE_TILES):
            put(14 + tile, final_ref[:, tile * LANES : (tile + 1) * LANES])
        put(13, jnp.concatenate([ada_ref[0, :, 13 * LANES : 13 * LANES + 64], blank], axis=1))

    @pl.when(side == 1)
    def _():
        put(MOD_TILES - 1, jnp.concatenate([blank, ada_ref[0, :, 0:64]], axis=1))
        for tile in range(1, 14):
            start = tile * LANES - 64
            put(22 + tile, ada_ref[0, :, start : start + LANES])
        for tile in range(FEATURE_TILES):
            put(36 + tile, final_ref[:, tile * LANES : (tile + 1) * LANES])

    for slot in (0, 1, 4):
        small[slot].wait()
    time_now = jnp.full((1, LANES), now_ref[side], F32)
    step_size = jnp.full((1, LANES), step_ref[side], F32)
    later = time_now - step_size
    moments = jnp.concatenate([time_now, later, jnp.zeros((6, LANES), F32)], axis=0)

    def condition():
        index = lanes_of((8, LANES)).astype(F32)
        rates = jnp.exp(-math.log(10000.0) * index / (FREQ // 2))
        angles = 1000.0 * moments * rates
        features = jnp.concatenate([jnp.cos(angles), jnp.sin(angles)], axis=1).astype(BF16)
        loads[0].wait()
        hidden = silu(dot(features, time_in[...])).astype(BF16)
        loads[1].wait()
        loads[2].start()
        loads[3].start()
        label = own_row(labels_ref[...].astype(F32))
        cond = silu(label + dot(hidden, time_out[...])).astype(BF16)
        for tile in range(FEATURE_TILES):
            piece = cond[0:2, tile * LANES : (tile + 1) * LANES]
            cond_send[tile] = piece
            cond_all[me, tile] = piece

    early = me < CHIPS // 2
    pl.when(early)(condition)

    @pl.when(holder)
    def _():
        pl.semaphore_wait(barrier, MOD_TILES)

    @pl.when(jnp.logical_not(holder))
    def _():
        pl.semaphore_wait(barrier, MOD_TILES + 1)

    base = side * SIDE_TILES
    direct = jnp.logical_and(me >= base, me < base + SIDE_TILES)

    def send_tile(step):
        chip = base + lax.rem(me + step, SIDE_TILES)
        pltpu.make_async_remote_copy(
            src_ref=stage.at[chip],
            dst_ref=tiles_all.at[pl.ds(me * 9, 9)],
            send_sem=weight_sem.at[0],
            recv_sem=weight_sem.at[1],
            device_id=at(chip, side),
            device_id_type=MESH,
        ).start()

    def send_rows(step):
        pltpu.make_async_remote_copy(
            src_ref=cond_send,
            dst_ref=cond_all.at[me],
            send_sem=cond_sem.at[0],
            recv_sem=cond_sem.at[1],
            device_id=at(lax.rem(me + step, MOD_TILES), side),
            device_id_type=MESH,
        ).start()

    for step in range(1, SIDE_TILES):
        send_tile(step)

    @pl.when(jnp.logical_not(direct))
    def _():
        send_tile(0)

    @pl.when(direct)
    def _():
        tiles_all[pl.ds(me * 9, 9)] = stage[me]

    pl.when(jnp.logical_not(early))(condition)

    for step in range(1, MOD_TILES):
        send_rows(step)

    @pl.when(jnp.logical_not(holder))
    def _():
        send_rows(0)

    tile_share = pltpu.make_async_remote_copy(
        src_ref=tiles_all,
        dst_ref=tiles_all,
        send_sem=tile_sem.at[0],
        recv_sem=tile_sem.at[1],
        device_id=at(me, other),
        device_id_type=MESH,
    )

    swaps = []
    for slot, (src, dst) in enumerate(((qkv_ref, wqkv.at[:, side]), (out_ref, wout.at[own_half]))):
        swaps.append(
            pltpu.make_async_remote_copy(
                src_ref=src,
                dst_ref=dst,
                send_sem=swap_sem.at[slot],
                recv_sem=swap_sem.at[2 + slot],
                device_id=at(me, other),
                device_id_type=MESH,
            )
        )
        swaps[-1].start()

    for copy in small[5:]:
        copy.wait()
    lane8 = lanes_of((CHUNK_ROWS, LANES)) // PATCH_VALS
    for piece in range(CHUNK_ROWS):
        span = slice(piece * LANES, (piece + 1) * LANES)
        rows[0, piece : piece + 1, :] = own_row(current_ref[:, span])
        rows[1, piece : piece + 1, :] = own_row(noise_ref[:, span])
    current = rows[0]
    draw = rows[1]
    for copy in range(PER_ROW):
        patch8[copy * PATCH_VALS : (copy + 1) * PATCH_VALS, :] = patch_ref[...]
    spread_lanes = (
        lax.broadcasted_iota(jnp.int32, (LANES, PATCH_VALS), 0) % PATCH_VALS
        == lanes_of((LANES, PATCH_VALS))
    )
    proj8[...] = dot(jnp.where(spread_lanes, 1.0, 0.0).astype(BF16), proj_ref[...]).astype(BF16)

    half = D // 2
    queries[...] = jnp.zeros_like(queries)

    def table_chunk(j, carry):
        place = lax.broadcasted_iota(jnp.int32, (CHUNK_ROWS, D), 0) * PER_ROW + j
        column = lanes_of((CHUNK_ROWS, D))
        first = column < half
        freq = jnp.where(first, column, column - half).astype(F32)
        angle = place.astype(F32) * jnp.exp(-math.log(10000.0) * freq / half)
        table[pl.ds(pl.multiple_of(j * CHUNK_ROWS, CHUNK_ROWS), CHUNK_ROWS), :] = jnp.where(
            first, jnp.sin(angle), jnp.cos(angle)
        )
        return carry

    lax.fori_loop(0, PER_ROW, table_chunk, 0)

    spans = [slice(j * CHUNK_ROWS, (j + 1) * CHUNK_ROWS) for j in range(PER_ROW)]

    def prepare(latent):
        tokens = jnp.concatenate(
            [jnp.where(lane8 == j, latent, 0.0) for j in range(PER_ROW)], axis=0
        ).astype(BF16)
        stream[...] = dot(tokens, patch8[...]) + table[...]
        means, spreads = moments_of(stream, spans)
        for span, mean, scale in zip(spans, means, spreads):
            unit[span] = (stream[span] - mean) * scale

    prepare(current)

    def drain(ref, sem):
        pltpu.make_async_copy(ref, ref, sem).wait()

    relay = jnp.logical_and(holder, jnp.logical_not(direct))

    @pl.when(direct)
    def _():
        drain(tiles_all.at[pl.ds(0, 9 * (CHIPS - 1))], weight_sem.at[1])
        tile_share.start()

    @pl.when(holder)
    def _():
        drain(cond_all.at[pl.ds(0, CHIPS - 1)], cond_sem.at[1])

    @pl.when(relay)
    def _():
        tile_share.wait_recv()

    @pl.when(holder)
    def _():
        total = jnp.zeros((2 * CHIPS, LANES), F32)
        for tile in range(FEATURE_TILES):
            lhs = cond_all[:, tile].reshape(2 * CHIPS, LANES)
            rhs = tiles_all[tile * 64 : (tile + 1) * 64].reshape(LANES, LANES)
            total = total + dot(lhs, rhs)
        mod_send[...] = total.reshape(CHIPS, 2, LANES)
        mods[me] = mod_send[me]

        for chip in peers:
            pltpu.make_async_remote_copy(
                src_ref=mod_send.at[chip],
                dst_ref=mods.at[me],
                send_sem=mod_sem.at[0],
                recv_sem=mod_sem.at[1],
                device_id=at(chip, side),
                device_id_type=MESH,
            ).start()

    @pl.when(holder)
    def _():
        drain(mods.at[pl.ds(0, MOD_TILES - 1)], mod_sem.at[1])

    @pl.when(me >= MOD_TILES)
    def _():
        drain(mods, mod_sem.at[1])

    loads[2].wait()
    loads[3].wait()
    for swap in swaps:
        swap.wait()

    def mod_row(which, moment):
        tiles = [mods[chip] + mods[45] if chip == 13 else mods[chip] for chip in TILE_CHIPS[which]]
        pair = jnp.concatenate(tiles, axis=1)
        return jnp.where(moment == 0, pair[0:1], pair[1:2])

    nothing = jnp.zeros((8, TOK), F32)
    exponent = HEAD_DIM ** (-0.5) * math.log2(math.e)

    def evaluate(moment):
        shift, scale = mod_row(0, moment), 1.0 + mod_row(1, moment)
        for span in spans:
            normal[span] = (unit[span] * scale + shift).astype(BF16)

        turned[...] = normal[...].T
        keys[...] = dot(wqkv[1].reshape(D, D), turned[...]).astype(BF16).T

        def project(four):
            group, row = four // 2, four % 2 * FOUR
            asked = dot(wqkv[0, group, row : row + FOUR], turned[...]) * exponent
            given = dot(wqkv[2, group, row : row + FOUR], turned[...])
            for place in range(4):
                head = 4 * four + place
                low = head * HEAD_DIM
                span = slice(place * HEAD_DIM, (place + 1) * HEAD_DIM)
                rows72 = [asked[span], nothing] if low % 16 == 0 else [nothing, asked[span]]
                start = low // 16 * 16 - low // LANES * LANES
                queries[head, start : start + 80] = jnp.concatenate(rows72, axis=0).astype(BF16)
                values[head] = jnp.concatenate([given[span], nothing + 1.0], axis=0).astype(BF16)

        def leave():
            return lax.dot_general(
                mixed[...].astype(BF16),
                wout[...],
                (((0,), (0,)), ((), ())),
                preferred_element_type=F32,
            )

        def score(head):
            low, high = head * HEAD_DIM, (head + 1) * HEAD_DIM
            left = low // LANES * LANES
            right = -(-high // LANES) * LANES
            scores[head % 2] = dot(keys[:, left:right], queries[head, : right - left])

        def soften(head):
            found = scores[head % 2]
            weights = jnp.exp2(found - jnp.max(found, axis=0, keepdims=True))
            probs[head % 2] = weights.astype(BF16)

        def apply(head):
            result = dot(values[head], probs[head % 2])
            mixed[head * HEAD_DIM : (head + 1) * HEAD_DIM] = result[:HEAD_DIM] * (
                1.0 / result[HEAD_DIM : HEAD_DIM + 1]
            )

        project(0)
        score(0)
        for head in range(HEADS):
            if head % 4 == 0 and head + 4 < HEADS:
                project(head // 4 + 1)
            if head + 1 < HEADS:
                score(head + 1)
            soften(head)
            if head:
                apply(head - 1)
        apply(HEADS - 1)
        stream[...] = stream[...] + mod_row(2, moment) * leave()
        shift, scale = mod_row(3, moment), 1.0 + mod_row(4, moment)
        means, spreads = moments_of(stream, spans)
        for span, mean, spread_inv in zip(spans, means, spreads):
            normal[span] = ((stream[span] - mean) * spread_inv * scale + shift).astype(BF16)
        guessed = dot_t(normal[...], proj8[...])
        result = jnp.zeros((CHUNK_ROWS, LANES), F32)
        for j in range(PER_ROW):
            result = result + jnp.where(
                lane8 == j, guessed[j * CHUNK_ROWS : (j + 1) * CHUNK_ROWS], 0.0
            )
        return result

    spread = jnp.sqrt(step_size * beta_at(time_now)) * draw


    def one_moment(moment, carry):
        guess = evaluate(moment)
        rows[4] = guess

        @pl.when(moment == 0)
        def _():
            rows[3] = guess
            beta = beta_at(time_now)
            drift_now = 0.5 * beta * rows[0] - beta * guess / sigma_at(time_now)
            euler_now = rows[0] + step_size * drift_now + spread
            rows[2] = euler_now
            prepare(euler_now)

        return carry

    lax.fori_loop(0, 2, one_moment, 0)

    current = rows[0]
    beta = beta_at(time_now)
    drift_now = 0.5 * beta * current - beta * rows[3] / sigma_at(time_now)
    euler = rows[2]
    beta_then = beta_at(later)
    drift_later = 0.5 * beta_then * euler - beta_then * rows[4] / sigma_at(later)
    heun = current + 0.5 * step_size * (drift_now + drift_later) + spread
    scale_ref = jnp.maximum(tol_abs, tol_rel * jnp.maximum(jnp.abs(heun), jnp.abs(current)))
    gap = (euler - heun) / scale_ref
    squares = jnp.sum(jnp.sum(gap * gap, axis=1, keepdims=True), axis=0, keepdims=True)
    error = jnp.sqrt(squares / LATENT)
    taken = jnp.full((CHUNK_ROWS, LANES), accept_ref[side], jnp.int32) == 1
    finals[side, :CHUNK_ROWS] = jnp.where(taken, heun, current)
    finals[side, CHUNK_ROWS:] = jnp.broadcast_to(error, (8, LANES))
    final_swap = pltpu.make_async_remote_copy(
        src_ref=finals.at[side],
        dst_ref=finals.at[side],
        send_sem=final_sem.at[0],
        recv_sem=final_sem.at[1],
        device_id=at(me, other),
        device_id_type=MESH,
    )
    final_swap.start()

    @pl.when(me >= MOD_TILES)
    def _():
        drain(cond_all.at[pl.ds(0, MOD_TILES)], cond_sem.at[0])

    @pl.when(me < MOD_TILES)
    def _():
        drain(cond_all.at[pl.ds(0, MOD_TILES - 1)], cond_sem.at[0])
        drain(mod_send.at[pl.ds(0, CHIPS - 1)], mod_sem.at[0])

    @pl.when(direct)
    def _():
        drain(tiles_all.at[pl.ds(0, 9 * (SIDE_TILES - 1))], weight_sem.at[0])
        tile_share.wait_send()

    @pl.when(jnp.logical_not(direct))
    def _():
        drain(tiles_all.at[pl.ds(0, 9 * SIDE_TILES)], weight_sem.at[0])

    final_swap.wait()
    for latent in range(2):
        for piece in range(CHUNK_ROWS):
            state_ref[latent : latent + 1, piece * LANES : (piece + 1) * LANES] = finals[
                latent, piece : piece + 1, :
            ]
    pair = jnp.where(
        lanes_of((1, LANES)) == 0,
        finals[0, CHUNK_ROWS : CHUNK_ROWS + 1, :],
        finals[1, CHUNK_ROWS : CHUNK_ROWS + 1, :],
    )
    error_ref[...] = pair[0, :2]


def shards(
    current,
    noise_draw,
    labels,
    time_now,
    step_size,
    accept,
    patch_weight,
    time_in,
    time_out,
    qkv_weight,
    out_weight,
    ada_weight,
    final_ada,
    final_proj,
):
    vmem = pl.BlockSpec(memory_space=pltpu.VMEM)
    place = pl.BlockSpec(memory_space=pl.ANY)
    state, error = pl.pallas_call(
        kernel,
        out_shape=(
            pltpu.VMEM((2, LATENT), F32),
            pltpu.VMEM((2,), F32),
        ),
        in_specs=[place] * 14,
        out_specs=(vmem, vmem),
        scratch_shapes=[
            pltpu.SMEM((2,), F32),
            pltpu.SMEM((2,), F32),
            pltpu.SMEM((2,), jnp.int32),
            pltpu.VMEM((2, LATENT), F32),
            pltpu.VMEM((2, LATENT), F32),
            pltpu.VMEM((2, D), BF16),
            pltpu.VMEM((PATCH_VALS, D), BF16),
            pltpu.VMEM((PATCH_VALS, D), BF16),
            pltpu.VMEM((1, 18, 3 * HALF), BF16),
            pltpu.VMEM((18, D), BF16),
            pltpu.VMEM((FREQ, D), BF16),
            pltpu.VMEM((D, D), BF16),
            pltpu.VMEM((3, GROUPS, HALF, D), BF16),
            pltpu.VMEM((D, D), BF16),
            pltpu.VMEM((MOD_TILES, 9, 2, LANES), BF16),
            pltpu.VMEM((FEATURE_TILES, 2, LANES), BF16),
            pltpu.VMEM((CHIPS, FEATURE_TILES, 2, LANES), BF16),
            pltpu.VMEM((9 * CHIPS, 2, LANES), BF16),
            pltpu.VMEM((CHIPS, 2, LANES), F32),
            pltpu.VMEM((MOD_TILES, 2, LANES), F32),
            pltpu.VMEM((2, CHUNK_ROWS + 8, LANES), F32),
            pltpu.VMEM((LANES, D), BF16),
            pltpu.VMEM((LANES, D), BF16),
            pltpu.VMEM((TOK, D), F32),
            pltpu.VMEM((TOK, D), F32),
            pltpu.VMEM((TOK, D), F32),
            pltpu.VMEM((TOK, D), BF16),
            pltpu.VMEM((HEADS, 2 * LANES, TOK), BF16),
            pltpu.VMEM((TOK, D), BF16),
            pltpu.VMEM((HEADS, 80, TOK), BF16),
            pltpu.VMEM((D, TOK), F32),
            pltpu.VMEM((D, TOK), BF16),
            pltpu.VMEM((2, TOK, TOK), F32),
            pltpu.VMEM((2, TOK, TOK), BF16),
            pltpu.VMEM((5, CHUNK_ROWS, LANES), F32),
            pltpu.SemaphoreType.DMA((4,)),
            pltpu.SemaphoreType.DMA((10,)),
            pltpu.SemaphoreType.DMA((2,)),
            pltpu.SemaphoreType.DMA((4,)),
            pltpu.SemaphoreType.DMA((2,)),
            pltpu.SemaphoreType.DMA((2,)),
            pltpu.SemaphoreType.DMA((2,)),
            pltpu.SemaphoreType.DMA((2,)),
        ],
        compiler_params=pltpu.CompilerParams(
            collective_id=0, has_side_effects=True, vmem_limit_bytes=60 * 1024 * 1024
        ),
        name="heun_step",
    )(
        time_now,
        step_size,
        accept,
        current,
        noise_draw,
        labels,
        patch_weight,
        final_proj.T,
        ada_weight,
        final_ada,
        time_in,
        time_out,
        qkv_weight[0].transpose(1, 2, 0),
        out_weight[0].T,
    )
    return state, error


def solution(mesh):
    in_specs = (
        P("dp", None),
        P("dp", None),
        P("dp", None),
        P("dp"),
        P("dp"),
        P("dp"),
        P(),
        P(),
        P(),
        P(None, None, None, "tensor"),
        P(None, None, "tensor"),
        P(None, "dp", "tensor"),
        P("dp", "tensor"),
        P(),
    )
    out_specs = (P("dp", None), P("dp"))
    return jax.shard_map(shards, mesh=mesh, in_specs=in_specs, out_specs=out_specs, check_vma=False)
```
